256 devices in a mesh: shot: 4 (over x_lo, core), tile: 64 (over x_hi, z, y).
Axes of the slice: x: 4 (x_hi: 2, x_lo: 2; x = x_hi * 2 + x_lo), y: 4, z: 8, core: 2. Of those that a mesh axis runs over, the one named last changes fastest.
Arguments:
- partials: bfloat16 [256, 8, 512, 512], P(('shot', 'tile')), may hold values from -6 to 6
Outputs:
- filtered: float32 [8, 512, 512], P('shot', 'tile')
The draws below stay inside these ranges and needn't reach their ends.
All inputs are finite; a program needn't handle non-finite values.
Results may differ from the reference program's by a relative error of at most 0.0003.
Values may be sent and summed in bfloat16 or wider, within the bound.
A program may use at most 64 MiB of HBM per device.

```python
import jax
import jax.numpy as jnp
from jax import lax

DEPTH = 8
NX = 512
NY = 512
SHOTS = 256


def block_scale(key, shape, shards, low, high):
    level = 1.0
    for dim, blocks in shards:
        draws = jax.random.uniform(jax.random.fold_in(jax.random.fold_in(key, 6), dim), (blocks,), jnp.float32, low / len(shards), high / len(shards))
        level = level * jnp.repeat(jnp.exp(draws), shape[dim] // blocks).reshape((-1,) + (1,) * (len(shape) - 1 - dim))
    return level


def gaussian(own_key, extent, spread, bound, pieces=(), kind=jnp.bfloat16):
    result = jax.random.normal(own_key, extent, jnp.float32) * spread
    if len(pieces) > 0:
        result = block_scale(own_key, extent, pieces, -0.22, 0.18) * result
    return jnp.clip(result, min=-bound, max=bound).astype(kind)


def setup_inputs(seed: int = 0) -> dict:
    splits = jax.random.split(jax.random.key(seed), 2)
    return {
        "partials": gaussian(splits[0], (SHOTS, DEPTH, NX, NY), 1.0, 6.0, ((0, 256),)),
    }


def reference(partials):

    def add_one(total, piece):
        return (total + piece.astype(jnp.float32), None)
    start = jnp.zeros((DEPTH, NX, NY), jnp.float32)
    stack, unused = lax.scan(add_one, start, partials)
    image = stack / jnp.sqrt(jnp.float32(SHOTS))
    padded = jnp.pad(image, 1)
    beside = padded[2:, 1:-1, 1:-1] + padded[:-2, 1:-1, 1:-1]
    beside = beside + padded[1:-1, 2:, 1:-1] + padded[1:-1, :-2, 1:-1]
    beside = beside + padded[1:-1, 1:-1, 2:] + padded[1:-1, 1:-1, :-2]
    return 6.0 * image - beside
```

```python
import functools

import jax
import jax.numpy as jnp
from jax import lax
from jax.experimental import pallas as pl
from jax.experimental.pallas import tpu as pltpu
from jax.sharding import PartitionSpec as P

MESH = pl.DeviceIdType.MESH
NCH = 2
NY = 512
CW = NY // NCH
F32 = jnp.float32
BF16 = jnp.bfloat16


def kernel(scale, pa, pb, out, own, sib, rel, dirt, cout, cin, S, qrel, qdir, qout, qin, T, zin, img, rows, deps,
           own_sem, sib_s, sib_r, rel_s, rel_r, dir_s, dir_r, c_s, c_r, qrel_s, qrel_r, qdir_s, qdir_r, qc_s, qc_r,
           z_s, z_r, row_s, row_r, dep_s, dep_r):
    s, t = lax.axis_index("shot"), lax.axis_index("tile")
    core, xl = lax.rem(s, 2), s // 2
    xh, z, y = t // 32, lax.rem(t // 4, 8), lax.rem(t, 4)
    X = xh * 2 + xl

    def at(Xq, zq, yq, cq):
        return (lax.rem(Xq, 2) * 2 + cq, (Xq // 2) * 32 + zq * 4 + yq)

    def wrap(v, n):
        return lax.rem(v + n, n)

    def peer(g, step, cq):
        if g == 0:
            return at(wrap(X + step, 4), z, y, cq)
        return at(X, z, wrap(y + step, 4), cq)

    other = 1 - core
    ring = lambda d, n, p: lax.rem(p + d + n, n)
    neighbours = [(s + 1 - 2 * core, t)]
    for g in range(2):
        for step in (1, -1):
            for cq in range(2):
                neighbours.append(peer(g, step, cq))
    for k in range(1, 8):
        neighbours.append(at(X, ring(k, 8, z), y, core))
    neighbours.append((s, ring(1, 64, t)))
    neighbours.append((s, ring(-1, 64, t)))
    barrier = pltpu.get_barrier_semaphore()
    for dev in neighbours:
        pl.semaphore_signal(barrier, inc=1, device_id=dev, device_id_type=MESH)
    pl.semaphore_wait(barrier, len(neighbours))

    sends = []

    def send(src, dst, ss, rs, dev):
        cp = pltpu.make_async_remote_copy(src_ref=src, dst_ref=dst, send_sem=ss, recv_sem=rs, device_id=dev,
                                          device_id_type=MESH)
        cp.start()
        sends.append(cp)
        return cp

    def wait_in(dst, rs):
        pltpu.make_async_copy(dst, dst, rs).wait()

    def raw(g, ch, step, cq, h):
        cols = pl.ds(ch * CW, CW)
        if g == 0:
            Xq = wrap(X + step, 4)
            return pa.at[2 * (lax.rem(Xq, 2) * 2 + cq), pl.ds(32 * (Xq // 2) + 16 * h, 16), :, cols]
        return pb.at[2 * (h * 2 + cq) + 1, :, wrap(y + step, 4), :, cols]

    PIECES = ((1, 0), (-1, 1), (0, 0), (0, 1))

    def raw_relay(g, ch):
        for d, step in enumerate((1, -1)):
            for cq in range(2):
                send(raw(g, ch, 2, cq, d), rel.at[g, ch, d, core], rel_s.at[g, ch, d, cq], rel_r.at[g, ch, d, core],
                     peer(g, step, cq))

    def raw_direct(g, ch):
        for d, step in enumerate((1, -1)):
            for cq in range(2):
                send(raw(g, ch, step, cq, 1 - d), dirt.at[g, ch, d, core], dir_s.at[g, ch, d, cq],
                     dir_r.at[g, ch, d, core], peer(g, step, cq))

    def raw_pair(g, ch):
        for i, (step, h) in enumerate(PIECES):
            pltpu.make_async_copy(raw(g, ch, step, core, h), own.at[g, ch, i], own_sem.at[g, ch, i]).start()
            send(raw(g, ch, step, other, h), sib.at[g, ch, i], sib_s.at[g, ch, i], sib_r.at[g, ch, i],
                 (s + 1 - 2 * core, t))

    def wait_pair(g, ch, i):
        wait_in(own.at[g, ch, i], own_sem.at[g, ch, i])
        wait_in(sib.at[g, ch, i], sib_r.at[g, ch, i])

    def add(ref, *idx):
        return ref[idx].astype(F32)

    def combine(g, ch):
        for d, step in enumerate((1, -1)):
            wait_pair(g, ch, d)
            for cq in range(2):
                wait_in(rel.at[g, ch, d, cq], rel_r.at[g, ch, d, cq])

            @pl.loop(0, 16)
            def _(i):
                cout[g, ch, d, i] = (add(own, g, ch, d, i) + add(sib, g, ch, d, i)) + (
                    add(rel, g, ch, d, 0, i) + add(rel, g, ch, d, 1, i))

            send(cout.at[g, ch, d], cin.at[g, ch, d], c_s.at[g, ch, d], c_r.at[g, ch, d], peer(g, step, core))

    def first_sum(g, ch):
        for h in range(2):
            wait_pair(g, ch, 2 + h)
            for cq in range(2):
                wait_in(dirt.at[g, ch, 1 - h, cq], dir_r.at[g, ch, 1 - h, cq])
            wait_in(cin.at[g, ch, h], c_r.at[g, ch, h])

            @pl.loop(0, 4)
            def _(i):
                for j in range(4):
                    k = i * 4 + j
                    S[g, ch, h, i, j] = ((add(own, g, ch, 2 + h, k) + add(sib, g, ch, 2 + h, k)) + (
                        add(dirt, g, ch, 1 - h, 0, k) + add(dirt, g, ch, 1 - h, 1, k))) + cin[g, ch, h, k]

    def qblock(g, ch, step, h):
        if g == 0:
            return S.at[g, ch, h, :, wrap(y + step, 4)]
        Xq = wrap(X + step, 4)
        return S.at[g, ch, lax.rem(Xq, 2), (Xq // 2) * 2 + h]

    def second_raw(g, ch):
        for d, step in enumerate((1, -1)):
            dev = peer(1 - g, step, core)
            send(qblock(g, ch, 2, d), qrel.at[g, ch, d], qrel_s.at[g, ch, d], qrel_r.at[g, ch, d], dev)
        for d, step in enumerate((1, -1)):
            dev = peer(1 - g, step, core)
            send(qblock(g, ch, step, 1 - d), qdir.at[g, ch, d], qdir_s.at[g, ch, d], qdir_r.at[g, ch, d], dev)

    def second_combine(g, ch):
        for d, step in enumerate((1, -1)):
            wait_in(qrel.at[g, ch, d], qrel_r.at[g, ch, d])
            qout[g, ch, d] = qrel[g, ch, d] + qblock(g, ch, step, d)[...]
            send(qout.at[g, ch, d], qin.at[g, ch, d], qc_s.at[g, ch, d], qc_r.at[g, ch, d], peer(1 - g, step, core))

    def second_sum(g, ch):
        for h in range(2):
            wait_in(qdir.at[g, ch, 1 - h], qdir_r.at[g, ch, 1 - h])
            wait_in(qin.at[g, ch, h], qc_r.at[g, ch, h])
            total = (qdir[g, ch, 1 - h] + qin[g, ch, h]) + qblock(g, ch, 0, h)[...]
            for j in range(4):
                T[ch, 4 * h + j, g] = total[j]

    def third_send(ch):
        for k in range(1, 8):
            zq = ring(k, 8, z)
            send(T.at[ch, zq], zin.at[ch, k - 1], z_s.at[ch, k - 1], z_r.at[ch, k - 1], at(X, zq, y, core))

    def third_sum(ch):
        total = T[ch, z]
        for k in range(1, 8):
            wait_in(zin.at[ch, k - 1], z_r.at[ch, k - 1])
            total = total + zin[ch, k - 1]
        img[:, :, ch * CW:(ch + 1) * CW] = total * scale

    both = ((0,), (1,))
    for g in range(2):
        raw_relay(g, 0)
    for g in range(2):
        raw_pair(g, 0)
    for g in range(2):
        raw_direct(g, 0)
    for ch in range(1, NCH):
        for g in range(2):
            raw_relay(g, ch)
        for g in range(2):
            raw_pair(g, ch)
    for ch in range(NCH):
        for g in range(2):
            combine(g, ch)
        if ch + 1 < NCH:
            for g in range(2):
                raw_direct(g, ch + 1)
        for g in range(2):
            first_sum(g, ch)
            second_raw(g, ch)
        for g in range(2):
            second_combine(g, ch)
        for g in range(2):
            second_sum(g, ch)
        third_send(ch)
    for ch in range(NCH):
        third_sum(ch)

    for d, step in enumerate((1, -1)):
        send(img, rows.at[d], row_s.at[d], row_r.at[d], (s, ring(step, 64, t)))
        send(img.at[1 - d], deps.at[d], dep_s.at[d], dep_r.at[d], (ring(step, 4, s), t))

    for d in range(2):
        wait_in(rows.at[d], row_r.at[d])
        wait_in(deps.at[d], dep_r.at[d])
    below = jnp.where(s > 0, 1.0, 0.0).astype(F32)
    above = jnp.where(s < 3, 1.0, 0.0).astype(F32)
    left = jnp.where(t > 0, 1.0, 0.0).astype(F32)
    right = jnp.where(t < 63, 1.0, 0.0).astype(F32)
    lane = lax.broadcasted_iota(jnp.int32, (8, NY), 1)
    for p in range(2):
        v = img[p]
        if p == 0:
            beside = deps[0] * below + img[1]
        else:
            beside = deps[1] * above + img[0]
        prev = jnp.concatenate([rows[0, p, 7:8] * left, v[:7]], axis=0)
        following = jnp.concatenate([v[1:], rows[1, p, 0:1] * right], axis=0)
        beside = beside + prev + following
        beside = beside + jnp.where(lane == 0, 0.0, pltpu.roll(v, 1, 1))
        beside = beside + jnp.where(lane == NY - 1, 0.0, pltpu.roll(v, NY - 1, 1))
        out[p] = 6.0 * v - beside
    for cp in sends:
        cp.wait_send()


def solution(mesh):
    shots = mesh.shape["shot"] * mesh.shape["tile"]
    scale = 1.0 / float(shots) ** 0.5
    D = pltpu.SemaphoreType.DMA
    V = pltpu.VMEM

    def step(partials):
        pa = partials.reshape(8, 64, 8, NY)
        pb = partials.reshape(8, 16, 4, 8, NY)
        return pl.pallas_call(
            functools.partial(kernel, scale),
            out_shape=jax.ShapeDtypeStruct((2, 8, NY), F32),
            in_specs=[pl.BlockSpec(memory_space=pl.ANY)] * 2,
            out_specs=pl.BlockSpec(memory_space=pltpu.VMEM),
            scratch_shapes=[
                V((2, NCH, 4, 16, 8, CW), BF16),
                V((2, NCH, 4, 16, 8, CW), BF16),
                V((2, NCH, 2, 2, 16, 8, CW), BF16),
                V((2, NCH, 2, 2, 16, 8, CW), BF16),
                V((2, NCH, 2, 16, 8, CW), F32),
                V((2, NCH, 2, 16, 8, CW), F32),
                V((2, NCH, 2, 4, 4, 8, CW), F32),
                V((2, NCH, 2, 4, 8, CW), F32),
                V((2, NCH, 2, 4, 8, CW), F32),
                V((2, NCH, 2, 4, 8, CW), F32),
                V((2, NCH, 2, 4, 8, CW), F32),
                V((NCH, 8, 2, 8, CW), F32),
                V((NCH, 7, 2, 8, CW), F32),
                V((2, 8, NY), F32),
                V((2, 2, 8, NY), F32),
                V((2, 8, NY), F32),
                D((2, NCH, 4)),
                D((2, NCH, 4)), D((2, NCH, 4)),
                D((2, NCH, 2, 2)), D((2, NCH, 2, 2)),
                D((2, NCH, 2, 2)), D((2, NCH, 2, 2)),
                D((2, NCH, 2)), D((2, NCH, 2)),
                D((2, NCH, 2)), D((2, NCH, 2)),
                D((2, NCH, 2)), D((2, NCH, 2)),
                D((2, NCH, 2)), D((2, NCH, 2)),
                D((NCH, 7)), D((NCH, 7)),
                D((2,)), D((2,)),
                D((2,)), D((2,)),
            ],
            compiler_params=pltpu.CompilerParams(collective_id=0, has_side_effects=True,
                                                 vmem_limit_bytes=48 * 1024 * 1024),
        )(pa, pb)

    return jax.shard_map(step, mesh=mesh, in_specs=(P(("shot", "tile"), None, None, None),),
                         out_specs=P("shot", "tile", None), check_vma=False)
```

```python
import functools

import jax
import jax.numpy as jnp
from jax import lax
from jax.experimental import pallas as pl
from jax.experimental.pallas import tpu as pltpu
from jax.sharding import PartitionSpec as P

MESH = pl.DeviceIdType.MESH
NCH = 2
NY = 512
CW = NY // NCH
F32 = jnp.float32
BF16 = jnp.bfloat16


def kernel(scale, pa, pb, out, own, sib, rel, dirt, cout, cin, S, qrel, qdir, qout, qin, T, zin, img, rows, deps,
           own_sem, sib_s, sib_r, rel_s, rel_r, dir_s, dir_r, c_s, c_r, qrel_s, qrel_r, qdir_s, qdir_r, qc_s, qc_r,
           z_s, z_r, row_s, row_r, dep_s, dep_r):
    s, t = lax.axis_index("shot"), lax.axis_index("tile")
    core, xl = lax.rem(s, 2), s // 2
    xh, z, y = t // 32, lax.rem(t // 4, 8), lax.rem(t, 4)
    X = xh * 2 + xl

    def at(Xq, zq, yq, cq):
        return (lax.rem(Xq, 2) * 2 + cq, (Xq // 2) * 32 + zq * 4 + yq)

    def wrap(v, n):
        return lax.rem(v + n, n)

    def peer(g, step, cq):
        if g == 0:
            return at(wrap(X + step, 4), z, y, cq)
        return at(X, z, wrap(y + step, 4), cq)

    other = 1 - core
    ring = lambda d, n, p: lax.rem(p + d + n, n)
    neighbours = [(s + 1 - 2 * core, t)]
    for g in range(2):
        for step in (1, -1):
            for cq in range(2):
                neighbours.append(peer(g, step, cq))
    for k in range(1, 8):
        neighbours.append(at(X, ring(k, 8, z), y, core))
    neighbours.append((s, ring(1, 64, t)))
    neighbours.append((s, ring(-1, 64, t)))
    barrier = pltpu.get_barrier_semaphore()
    for dev in neighbours:
        pl.semaphore_signal(barrier, inc=1, device_id=dev, device_id_type=MESH)
    pl.semaphore_wait(barrier, len(neighbours))

    sends = []

    def send(src, dst, ss, rs, dev):
        cp = pltpu.make_async_remote_copy(src_ref=src, dst_ref=dst, send_sem=ss, recv_sem=rs, device_id=dev,
                                          device_id_type=MESH)
        cp.start()
        sends.append(cp)
        return cp

    def wait_in(dst, rs):
        pltpu.make_async_copy(dst, dst, rs).wait()

    def raw(g, ch, step, cq, h):
        cols = pl.ds(ch * CW, CW)
        if g == 0:
            Xq = wrap(X + step, 4)
            return pa.at[2 * (lax.rem(Xq, 2) * 2 + cq), pl.ds(32 * (Xq // 2) + 16 * h, 16), :, cols]
        return pb.at[2 * (h * 2 + cq) + 1, :, wrap(y + step, 4), :, cols]

    PIECES = ((1, 0), (-1, 1), (0, 0), (0, 1))

    def raw_relay(g, ch):
        for d, step in enumerate((1, -1)):
            for cq in range(2):
                send(raw(g, ch, 2, cq, d), rel.at[g, ch, d, core], rel_s.at[g, ch, d, cq], rel_r.at[g, ch, d, core],
                     peer(g, step, cq))

    def raw_direct(g, ch):
        for d, step in enumerate((1, -1)):
            for cq in range(2):
                send(raw(g, ch, step, cq, 1 - d), dirt.at[g, ch, d, core], dir_s.at[g, ch, d, cq],
                     dir_r.at[g, ch, d, core], peer(g, step, cq))

    def raw_pair(g, ch):
        for i, (step, h) in enumerate(PIECES):
            pltpu.make_async_copy(raw(g, ch, step, core, h), own.at[g, ch, i], own_sem.at[g, ch, i]).start()
            send(raw(g, ch, step, other, h), sib.at[g, ch, i], sib_s.at[g, ch, i], sib_r.at[g, ch, i],
                 (s + 1 - 2 * core, t))

    def wait_pair(g, ch, i):
        wait_in(own.at[g, ch, i], own_sem.at[g, ch, i])
        wait_in(sib.at[g, ch, i], sib_r.at[g, ch, i])

    def add(ref, *idx):
        return ref[idx].astype(F32)

    def combine(g, ch):
        for d, step in enumerate((1, -1)):
            wait_pair(g, ch, d)
            for cq in range(2):
                wait_in(rel.at[g, ch, d, cq], rel_r.at[g, ch, d, cq])

            @pl.loop(0, 16)
            def _(i):
                cout[g, ch, d, i] = (add(own, g, ch, d, i) + add(sib, g, ch, d, i)) + (
                    add(rel, g, ch, d, 0, i) + add(rel, g, ch, d, 1, i))

            send(cout.at[g, ch, d], cin.at[g, ch, d], c_s.at[g, ch, d], c_r.at[g, ch, d], peer(g, step, core))

    def first_sum(g, ch):
        for h in range(2):
            wait_pair(g, ch, 2 + h)
            for cq in range(2):
                wait_in(dirt.at[g, ch, 1 - h, cq], dir_r.at[g, ch, 1 - h, cq])
            wait_in(cin.at[g, ch, h], c_r.at[g, ch, h])

            @pl.loop(0, 4)
            def _(i):
                for j in range(4):
                    k = i * 4 + j
                    S[g, ch, h, i, j] = ((add(own, g, ch, 2 + h, k) + add(sib, g, ch, 2 + h, k)) + (
                        add(dirt, g, ch, 1 - h, 0, k) + add(dirt, g, ch, 1 - h, 1, k))) + cin[g, ch, h, k]

    def qblock(g, ch, step, h):
        if g == 0:
            return S.at[g, ch, h, :, wrap(y + step, 4)]
        Xq = wrap(X + step, 4)
        return S.at[g, ch, lax.rem(Xq, 2), (Xq // 2) * 2 + h]

    def second_raw(g, ch):
        for d, step in enumerate((1, -1)):
            dev = peer(1 - g, step, core)
            send(qblock(g, ch, 2, d), qrel.at[g, ch, d], qrel_s.at[g, ch, d], qrel_r.at[g, ch, d], dev)
        for d, step in enumerate((1, -1)):
            dev = peer(1 - g, step, core)
            send(qblock(g, ch, step, 1 - d), qdir.at[g, ch, d], qdir_s.at[g, ch, d], qdir_r.at[g, ch, d], dev)

    def second_combine(g, ch):
        for d, step in enumerate((1, -1)):
            wait_in(qrel.at[g, ch, d], qrel_r.at[g, ch, d])
            qout[g, ch, d] = qrel[g, ch, d] + qblock(g, ch, step, d)[...]
            send(qout.at[g, ch, d], qin.at[g, ch, d], qc_s.at[g, ch, d], qc_r.at[g, ch, d], peer(1 - g, step, core))

    def second_sum(g, ch):
        for h in range(2):
            wait_in(qdir.at[g, ch, 1 - h], qdir_r.at[g, ch, 1 - h])
            wait_in(qin.at[g, ch, h], qc_r.at[g, ch, h])
            total = (qdir[g, ch, 1 - h] + qin[g, ch, h]) + qblock(g, ch, 0, h)[...]
            for j in range(4):
                T[ch, 4 * h + j, g] = total[j]

    def third_send(ch):
        for k in range(1, 8):
            zq = ring(k, 8, z)
            send(T.at[ch, zq], zin.at[ch, k - 1], z_s.at[ch, k - 1], z_r.at[ch, k - 1], at(X, zq, y, core))

    def third_sum(ch):
        total = T[ch, z]
        for k in range(1, 8):
            wait_in(zin.at[ch, k - 1], z_r.at[ch, k - 1])
            total = total + zin[ch, k - 1]
        img[:, :, ch * CW:(ch + 1) * CW] = total * scale

    def each(fn, ch):
        if 0 <= ch < NCH:
            for g in range(2):
                fn(g, ch)

    each(raw_relay, 0)
    each(raw_pair, 0)
    each(raw_direct, 0)
    for k in range(1, NCH + 5):
        each(raw_relay, k)
        each(raw_pair, k)
        each(combine, k - 1)
        each(raw_direct, k)
        each(first_sum, k - 2)
        each(second_raw, k - 2)
        each(second_combine, k - 3)
        each(second_sum, k - 4)
        if 0 <= k - 4 < NCH:
            third_send(k - 4)
    for ch in range(NCH):
        third_sum(ch)

    for d, step in enumerate((1, -1)):
        send(img, rows.at[d], row_s.at[d], row_r.at[d], (s, ring(step, 64, t)))
        send(img.at[1 - d], deps.at[d], dep_s.at[d], dep_r.at[d], (ring(step, 4, s), t))

    for d in range(2):
        wait_in(rows.at[d], row_r.at[d])
        wait_in(deps.at[d], dep_r.at[d])
    below = jnp.where(s > 0, 1.0, 0.0).astype(F32)
    above = jnp.where(s < 3, 1.0, 0.0).astype(F32)
    left = jnp.where(t > 0, 1.0, 0.0).astype(F32)
    right = jnp.where(t < 63, 1.0, 0.0).astype(F32)
    lane = lax.broadcasted_iota(jnp.int32, (8, NY), 1)
    for p in range(2):
        v = img[p]
        if p == 0:
            beside = deps[0] * below + img[1]
        else:
            beside = deps[1] * above + img[0]
        prev = jnp.concatenate([rows[0, p, 7:8] * left, v[:7]], axis=0)
        following = jnp.concatenate([v[1:], rows[1, p, 0:1] * right], axis=0)
        beside = beside + prev + following
        beside = beside + jnp.where(lane == 0, 0.0, pltpu.roll(v, 1, 1))
        beside = beside + jnp.where(lane == NY - 1, 0.0, pltpu.roll(v, NY - 1, 1))
        out[p] = 6.0 * v - beside
    for cp in sends:
        cp.wait_send()


def solution(mesh):
    shots = mesh.shape["shot"] * mesh.shape["tile"]
    scale = 1.0 / float(shots) ** 0.5
    D = pltpu.SemaphoreType.DMA
    V = pltpu.VMEM

    def step(partials):
        pa = partials.reshape(8, 64, 8, NY)
        pb = partials.reshape(8, 16, 4, 8, NY)
        return pl.pallas_call(
            functools.partial(kernel, scale),
            out_shape=jax.ShapeDtypeStruct((2, 8, NY), F32),
            in_specs=[pl.BlockSpec(memory_space=pl.ANY)] * 2,
            out_specs=pl.BlockSpec(memory_space=pltpu.VMEM),
            scratch_shapes=[
                V((2, NCH, 4, 16, 8, CW), BF16),
                V((2, NCH, 4, 16, 8, CW), BF16),
                V((2, NCH, 2, 2, 16, 8, CW), BF16),
                V((2, NCH, 2, 2, 16, 8, CW), BF16),
                V((2, NCH, 2, 16, 8, CW), F32),
                V((2, NCH, 2, 16, 8, CW), F32),
                V((2, NCH, 2, 4, 4, 8, CW), F32),
                V((2, NCH, 2, 4, 8, CW), F32),
                V((2, NCH, 2, 4, 8, CW), F32),
                V((2, NCH, 2, 4, 8, CW), F32),
                V((2, NCH, 2, 4, 8, CW), F32),
                V((NCH, 8, 2, 8, CW), F32),
                V((NCH, 7, 2, 8, CW), F32),
                V((2, 8, NY), F32),
                V((2, 2, 8, NY), F32),
                V((2, 8, NY), F32),
                D((2, NCH, 4)),
                D((2, NCH, 4)), D((2, NCH, 4)),
                D((2, NCH, 2, 2)), D((2, NCH, 2, 2)),
                D((2, NCH, 2, 2)), D((2, NCH, 2, 2)),
                D((2, NCH, 2)), D((2, NCH, 2)),
                D((2, NCH, 2)), D((2, NCH, 2)),
                D((2, NCH, 2)), D((2, NCH, 2)),
                D((2, NCH, 2)), D((2, NCH, 2)),
                D((NCH, 7)), D((NCH, 7)),
                D((2,)), D((2,)),
                D((2,)), D((2,)),
            ],
            compiler_params=pltpu.CompilerParams(collective_id=0, has_side_effects=True,
                                                 vmem_limit_bytes=48 * 1024 * 1024),
        )(pa, pb)

    return jax.shard_map(step, mesh=mesh, in_specs=(P(("shot", "tile"), None, None, None),),
                         out_specs=P("shot", "tile", None), check_vma=False)
```

```python
import functools

import jax
import jax.numpy as jnp
from jax import lax
from jax.experimental import pallas as pl
from jax.experimental.pallas import tpu as pltpu
from jax.sharding import PartitionSpec as P

MESH = pl.DeviceIdType.MESH
NCH = 4
NY = 512
CW = NY // NCH
F32 = jnp.float32
BF16 = jnp.bfloat16


def kernel(scale, pin, out, give, mine, theirs, psum, L, rel, dirt, cin, S, qrel, qdir, qin, T, zin,
           give_sem, mine_sem, th_s, th_r, rel_s, rel_r, dir_s, dir_r, c_s, c_r, qrel_s, qrel_r, qdir_s, qdir_r,
           qc_s, qc_r, z_s, z_r):
    s, t = lax.axis_index("shot"), lax.axis_index("tile")
    core, xl = lax.rem(s, 2), s // 2
    xh, z, y = t // 32, lax.rem(t // 4, 8), lax.rem(t, 4)
    X = xh * 2 + xl
    other = 1 - core
    zhalf = z // 4

    def at(Xq, zq, yq, cq):
        return (lax.rem(Xq, 2) * 2 + cq, (Xq // 2) * 32 + zq * 4 + yq)

    def wrap(v, n):
        return lax.rem(v + n, n)

    def pos(g, step):
        return wrap((X if g == 0 else y) + step, 4)

    def peer(g, step):
        return at(pos(0, step), z, y, core) if g == 0 else at(X, z, pos(1, step), core)

    sibling = at(X, z, y, other)

    def load(ch, half, dst, sem):
        cols = pl.ds(ch * CW, CW)
        for q in range(2):
            base = q * 32 + half * 16
            pltpu.make_async_copy(pin.at[:, pl.ds(base, 16), :, cols], dst.at[ch, :, q, pl.ds(1, 16)], sem.at[ch]).start()
            low = jnp.maximum(base - 1, 0)
            pltpu.make_async_copy(pin.at[:, pl.ds(low, 1), :, cols], dst.at[ch, :, q, pl.ds(0, 1)], sem.at[ch]).start()
            high = jnp.minimum(base + 16, 63)
            pltpu.make_async_copy(pin.at[:, pl.ds(high, 1), :, cols], dst.at[ch, :, q, pl.ds(17, 1)], sem.at[ch]).start()

    for ch in range(NCH):
        load(ch, other, give, give_sem)
        load(ch, core, mine, mine_sem)

    barrier = pltpu.get_barrier_semaphore()
    for dev in (sibling, peer(0, 1), peer(0, -1), peer(1, 1), peer(1, -1)):
        pl.semaphore_signal(barrier, inc=1, device_id=dev, device_id_type=MESH)
    for zq in range(8):
        @pl.when(jnp.logical_or(zhalf != core, zq != z))
        def _():
            pl.semaphore_signal(barrier, inc=1, device_id=at(X, zq, y, zhalf), device_id_type=MESH)
    for ch in range(NCH):
        for q in range(2):
            psum[ch, 0, q] = jnp.zeros((18, 8, CW), F32)
            psum[ch, 9, q] = jnp.zeros((18, 8, CW), F32)
    pl.semaphore_wait(barrier, 13 - jnp.where(zhalf == core, 1, 0))

    sends = []

    def send(src, dst, ss, rs, dev):
        cp = pltpu.make_async_remote_copy(src_ref=src, dst_ref=dst, send_sem=ss, recv_sem=rs, device_id=dev,
                                          device_id_type=MESH)
        cp.start()
        sends.append(cp)

    def wait_in(dst, rs):
        pltpu.make_async_copy(dst, dst, rs).wait()

    for ch in range(NCH):
        wait_in(give.at[ch], give_sem.at[ch])
        send(give.at[ch], theirs.at[ch], th_s.at[ch], th_r.at[ch], sibling)

    first = jnp.where(core == 0, 0.0, 1.0).astype(F32)
    last = jnp.where(core == 1, 0.0, 1.0).astype(F32)
    lane = lax.broadcasted_iota(jnp.int32, (64, CW), 1)

    def pair(ch):
        if not 0 <= ch < NCH:
            return
        wait_in(mine.at[ch], mine_sem.at[ch])
        wait_in(theirs.at[ch], th_r.at[ch])

        @pl.loop(0, 8)
        def _(d):
            for q in range(2):
                psum[ch, d + 1, q] = mine[ch, d, q].astype(F32) + theirs[ch, d, q].astype(F32)
            psum[ch, d + 1, 0, 0] = psum[ch, d + 1, 0, 0] * first
            psum[ch, d + 1, 1, 17] = psum[ch, d + 1, 1, 17] * last

    def stencil(ch, g):
        @pl.loop(0, 16)
        def _(i):
            q, xq, hf = i // 4, lax.rem(i // 2, 2), lax.rem(i, 2)
            d = 2 * q + g + 1
            mid = pl.ds(hf * 8 + 1, 8)
            w = psum[ch, d, xq, pl.ds(hf * 8, 10)].reshape(80, CW)
            c = w[8:72]
            n = (w[7:71] + w[9:73]) + (psum[ch, d - 1, xq, mid] + psum[ch, d + 1, xq, mid]).reshape(64, CW)
            before = pltpu.roll(psum[ch - 1, d, xq, mid].reshape(64, CW), 1, 1) if ch > 0 else 0.0
            after = pltpu.roll(psum[ch + 1, d, xq, mid].reshape(64, CW), CW - 1, 1) if ch < NCH - 1 else 0.0
            n = n + (jnp.where(lane == 0, before, pltpu.roll(c, 1, 1)) +
                     jnp.where(lane == CW - 1, after, pltpu.roll(c, CW - 1, 1)))
            r = (6.0 * c - n).reshape(8, 8, CW)
            if g == 0:
                L[0, ch, xq * 2 + q // 2, lax.rem(q, 2), pl.ds(hf * 8, 8)] = r
            else:
                for j in range(8):
                    L[1, ch, j % 4, lax.rem(q, 2), (q // 2) * 8 + xq * 4 + hf * 2 + j // 4] = r[j]

    DIRS = tuple(enumerate((1, -1)))

    def relay(g, ch):
        for d, step in DIRS:
            send(L.at[g, ch, pos(g, 2), d], rel.at[g, ch, d], rel_s.at[g, ch, d], rel_r.at[g, ch, d], peer(g, step))

    def direct(g, ch):
        for d, step in DIRS:
            send(L.at[g, ch, pos(g, step), 1 - d], dirt.at[g, ch, d], dir_s.at[g, ch, d], dir_r.at[g, ch, d],
                 peer(g, step))

    def combine(g, ch):
        for d, step in DIRS:
            wait_in(rel.at[g, ch, d], rel_r.at[g, ch, d])
            rel[g, ch, d] = rel[g, ch, d] + L[g, ch, pos(g, step), d]
            send(rel.at[g, ch, d], cin.at[g, ch, d], c_s.at[g, ch, d], c_r.at[g, ch, d], peer(g, step))

    def first_sum(g, ch):
        for h in range(2):
            wait_in(dirt.at[g, ch, 1 - h], dir_r.at[g, ch, 1 - h])
            wait_in(cin.at[g, ch, h], c_r.at[g, ch, h])
            total = (L[g, ch, pos(g, 0), h] + dirt[g, ch, 1 - h]) + cin[g, ch, h]
            for j in range(16):
                if g == 0:
                    S[g, ch, j % 4, h, j // 4] = total[j]
                else:
                    S[g, ch, (j // 4 % 2) * 2 + j // 8, h, j % 4] = total[j]

    def second_send(g, ch):
        o = 1 - g
        for d, step in DIRS:
            send(S.at[g, ch, pos(o, 2), d], qrel.at[g, ch, d], qrel_s.at[g, ch, d], qrel_r.at[g, ch, d], peer(o, step))
        for d, step in DIRS:
            send(S.at[g, ch, pos(o, step), 1 - d], qdir.at[g, ch, d], qdir_s.at[g, ch, d], qdir_r.at[g, ch, d],
                 peer(o, step))

    def second_combine(g, ch):
        o = 1 - g
        for d, step in DIRS:
            wait_in(qrel.at[g, ch, d], qrel_r.at[g, ch, d])
            qrel[g, ch, d] = qrel[g, ch, d] + S[g, ch, pos(o, step), d]
            send(qrel.at[g, ch, d], qin.at[g, ch, d], qc_s.at[g, ch, d], qc_r.at[g, ch, d], peer(o, step))

    def second_sum(g, ch):
        for h in range(2):
            wait_in(qdir.at[g, ch, 1 - h], qdir_r.at[g, ch, 1 - h])
            wait_in(qin.at[g, ch, h], qc_r.at[g, ch, h])
            total = (S[g, ch, pos(1 - g, 0), h] + qdir[g, ch, 1 - h]) + qin[g, ch, h]
            for j in range(4):
                T[ch, h, j, g] = total[j]

    zsends = []

    def third_send(ch):
        for k in range(4):
            j = lax.rem(z + k, 4)
            zq = core * 4 + j
            for cq in range(2):
                cp = pltpu.make_async_remote_copy(
                    src_ref=T.at[ch, cq, j], dst_ref=zin.at[ch, z], send_sem=z_s.at[ch, j, cq],
                    recv_sem=z_r.at[ch, z], device_id=at(X, zq, y, cq), device_id_type=MESH)
                remote = jnp.logical_or(zq != z, core != cq)
                zsends.append((cp, remote))

                @pl.when(remote)
                def _():
                    cp.start()

                @pl.when(jnp.logical_not(remote))
                def _():
                    zin[ch, z] = T[ch, cq, j]

    def third_sum(ch):
        for k in range(8):
            @pl.when(jnp.logical_or(zhalf != core, k != z))
            def _():
                wait_in(zin.at[ch, k], z_r.at[ch, k])
        total = (zin[ch, 0] + zin[ch, 1]) + (zin[ch, 2] + zin[ch, 3])
        total = total + ((zin[ch, 4] + zin[ch, 5]) + (zin[ch, 6] + zin[ch, 7]))
        out[:, :, ch * CW:(ch + 1) * CW] = total * scale

    def each(fn, ch):
        if 0 <= ch < NCH:
            for g in range(2):
                fn(g, ch)

    pair(0)
    for k in range(NCH + 4):
        pair(k + 1)
        if k < NCH:
            for g in range(2):
                stencil(k, g)
                relay(g, k)
        each(combine, k - 1)
        each(direct, k)
        each(first_sum, k - 2)
        each(second_send, k - 2)
        each(second_combine, k - 3)
        each(second_sum, k - 4)
        if 0 <= k - 4 < NCH:
            third_send(k - 4)
    for ch in range(NCH):
        third_sum(ch)
    for cp in sends:
        cp.wait_send()
    for cp, remote in zsends:
        @pl.when(remote)
        def _():
            cp.wait_send()


def solution(mesh):
    shots = mesh.shape["shot"] * mesh.shape["tile"]
    scale = 1.0 / float(shots) ** 0.5
    D = pltpu.SemaphoreType.DMA
    V = pltpu.VMEM

    def step(partials):
        return pl.pallas_call(
            functools.partial(kernel, scale),
            out_shape=jax.ShapeDtypeStruct((2, 8, NY), F32),
            in_specs=[pl.BlockSpec(memory_space=pl.ANY)],
            out_specs=pl.BlockSpec(memory_space=pltpu.VMEM),
            scratch_shapes=[
                V((NCH, 8, 2, 18, 8, CW), BF16),
                V((NCH, 8, 2, 18, 8, CW), BF16),
                V((NCH, 8, 2, 18, 8, CW), BF16),
                V((NCH, 10, 2, 18, 8, CW), F32),
                V((2, NCH, 4, 2, 16, 8, CW), F32),
                V((2, NCH, 2, 16, 8, CW), F32),
                V((2, NCH, 2, 16, 8, CW), F32),
                V((2, NCH, 2, 16, 8, CW), F32),
                V((2, NCH, 4, 2, 4, 8, CW), F32),
                V((2, NCH, 2, 4, 8, CW), F32),
                V((2, NCH, 2, 4, 8, CW), F32),
                V((2, NCH, 2, 4, 8, CW), F32),
                V((NCH, 2, 4, 2, 8, CW), F32),
                V((NCH, 8, 2, 8, CW), F32),
                D((NCH,)), D((NCH,)), D((NCH,)), D((NCH,)),
                D((2, NCH, 2)), D((2, NCH, 2)),
                D((2, NCH, 2)), D((2, NCH, 2)),
                D((2, NCH, 2)), D((2, NCH, 2)),
                D((2, NCH, 2)), D((2, NCH, 2)),
                D((2, NCH, 2)), D((2, NCH, 2)),
                D((2, NCH, 2)), D((2, NCH, 2)),
                D((NCH, 4, 2)), D((NCH, 8)),
            ],
            compiler_params=pltpu.CompilerParams(collective_id=0, has_side_effects=True,
                                                 vmem_limit_bytes=62 * 1024 * 1024),
        )(partials.reshape(8, 64, 8, NY))

    return jax.shard_map(step, mesh=mesh, in_specs=(P(("shot", "tile"), None, None, None),),
                         out_specs=P("shot", "tile", None), check_vma=False)
```

```python
import functools

import jax
import jax.numpy as jnp
from jax import lax
from jax.experimental import pallas as pl
from jax.experimental.pallas import tpu as pltpu
from jax.sharding import PartitionSpec as P

MESH = pl.DeviceIdType.MESH
NCH = 4
NY = 512
CW = NY // NCH
UNROLL = 2
STRAIGHT = (3,)
F32 = jnp.float32
BF16 = jnp.bfloat16


def kernel(scale, pin, out, give, mine, theirs, psum, L, rel, dirt, cin, S, qrel, qdir, qin, qall, T, zin,
           give_sem, mine_sem, th_s, th_r, rel_s, rel_r, dir_s, dir_r, c_s, c_r, qrel_s, qrel_r, qdir_s, qdir_r,
           qc_s, qc_r, qa_s, qa_r, z_s, z_r, tok):
    s, t = lax.axis_index("shot"), lax.axis_index("tile")
    core, xl = lax.rem(s, 2), s // 2
    xh, z, y = t // 32, lax.rem(t // 4, 8), lax.rem(t, 4)
    X = xh * 2 + xl
    other = 1 - core
    zhalf = z // 4

    def at(Xq, zq, yq, cq):
        return (lax.rem(Xq, 2) * 2 + cq, (Xq // 2) * 32 + zq * 4 + yq)

    def wrap(v, n):
        return lax.rem(v + n, n)

    def pos(g, step):
        return wrap((X if g == 0 else y) + step, 4)

    def peer(g, step):
        return at(pos(0, step), z, y, core) if g == 0 else at(X, z, pos(1, step), core)

    sibling = at(X, z, y, other)

    def load(ch, half, dst, sem):
        cols = pl.ds(ch * CW, CW)
        for q in range(2):
            base = q * 32 + half * 16
            pltpu.make_async_copy(pin.at[:, pl.ds(base, 16), :, cols], dst.at[ch, :, q, pl.ds(1, 16)], sem.at[ch]).start()
            low = jnp.maximum(base - 1, 0)
            pltpu.make_async_copy(pin.at[:, pl.ds(low, 1), :, cols], dst.at[ch, :, q, pl.ds(0, 1)], sem.at[ch]).start()
            high = jnp.minimum(base + 16, 63)
            pltpu.make_async_copy(pin.at[:, pl.ds(high, 1), :, cols], dst.at[ch, :, q, pl.ds(17, 1)], sem.at[ch]).start()

    for ch in range(NCH):
        load(ch, other, give, give_sem)
        load(ch, core, mine, mine_sem)

    zring = (at(X, wrap(z + 1, 8), y, core), at(X, wrap(z - 1, 8), y, core))
    barrier = pltpu.get_barrier_semaphore()
    for dev in (sibling, peer(0, 1), peer(0, -1), peer(1, 1), peer(1, -1), *zring):
        pl.semaphore_signal(barrier, inc=1, device_id=dev, device_id_type=MESH)
    for ch in range(NCH):
        for q in range(2):
            psum[ch, 0, q] = jnp.zeros((144, CW), F32)
            psum[ch, 9, q] = jnp.zeros((144, CW), F32)
    pl.semaphore_wait(barrier, 7)

    def token(k, devices):
        for dev in devices:
            pl.semaphore_signal(tok.at[k], inc=1, device_id=dev, device_id_type=MESH)

    def pass_token(k):
        pl.semaphore_wait(tok.at[k], 2 if k < 3 else 1)
        if k < 3:
            token(k + 1, zring if k < 2 else (sibling,))

    token(0, zring)

    sends = []

    def send(src, dst, ss, rs, dev):
        cp = pltpu.make_async_remote_copy(src_ref=src, dst_ref=dst, send_sem=ss, recv_sem=rs, device_id=dev,
                                          device_id_type=MESH)
        cp.start()
        sends.append(cp)

    def wait_in(dst, rs):
        pltpu.make_async_copy(dst, dst, rs).wait()

    for ch in range(NCH):
        wait_in(give.at[ch], give_sem.at[ch])
        send(give.at[ch], theirs.at[ch], th_s.at[ch], th_r.at[ch], sibling)

    first = jnp.where(core == 0, 0.0, 1.0).astype(F32)
    last = jnp.where(core == 1, 0.0, 1.0).astype(F32)
    lane = lax.broadcasted_iota(jnp.int32, (64, CW), 1)

    def pair(ch):
        if not 0 <= ch < NCH:
            return
        wait_in(mine.at[ch], mine_sem.at[ch])
        wait_in(theirs.at[ch], th_r.at[ch])

        @pl.loop(0, 8)
        def _(d):
            for q in range(2):
                psum[ch, d + 1, q] = (mine[ch, d, q].astype(F32) + theirs[ch, d, q].astype(F32)).reshape(144, CW)
            psum[ch, d + 1, 0, 0:8] = psum[ch, d + 1, 0, 0:8] * first
            psum[ch, d + 1, 1, 136:144] = psum[ch, d + 1, 1, 136:144] * last

    def stencil(ch, g):
        @pl.loop(0, 8, unroll=UNROLL)
        def _(i):
            q, xq = i // 2, lax.rem(i, 2)
            d = 2 * q + g + 1
            for hf in range(2):
                lo = hf * 64 + 8
                mid = slice(lo, lo + 64)
                c = psum[ch, d, xq, mid]
                before = psum[ch - 1, d, xq, mid] if ch > 0 else 0.0
                after = psum[ch + 1, d, xq, mid] if ch < NCH - 1 else 0.0
                n = psum[ch, d, xq, slice(lo - 1, lo + 63)] + psum[ch, d, xq, slice(lo + 1, lo + 65)]
                n = n + (psum[ch, d - 1, xq, mid] + psum[ch, d + 1, xq, mid])
                n = n + (pltpu.roll(jnp.where(lane == CW - 1, before, c), 1, 1) +
                         pltpu.roll(jnp.where(lane == 0, after, c), CW - 1, 1))
                r = (6.0 * c - n).reshape(8, 8, CW)
                if g == 0:
                    L[0, ch, xq * 2 + q // 2, lax.rem(q, 2), pl.ds(hf * 8, 8)] = r
                else:
                    for j in range(8):
                        L[1, ch, j % 4, lax.rem(q, 2), (q // 2) * 8 + xq * 4 + hf * 2 + j // 4] = r[j]

    DIRS = tuple(enumerate((1, -1)))

    def relay(g, ch):
        for d, step in DIRS:
            send(L.at[g, ch, pos(g, 2), d], rel.at[g, ch, d], rel_s.at[g, ch, d], rel_r.at[g, ch, d], peer(g, step))

    def direct(g, ch):
        for d, step in DIRS:
            send(L.at[g, ch, pos(g, step), 1 - d], dirt.at[g, ch, d], dir_s.at[g, ch, d], dir_r.at[g, ch, d],
                 peer(g, step))

    def combine(g, ch):
        for d, step in DIRS:
            wait_in(rel.at[g, ch, d], rel_r.at[g, ch, d])
            rel[g, ch, d] = rel[g, ch, d] + L[g, ch, pos(g, step), d]
            send(rel.at[g, ch, d], cin.at[g, ch, d], c_s.at[g, ch, d], c_r.at[g, ch, d], peer(g, step))

    def first_sum(g, ch):
        for h in range(2):
            wait_in(dirt.at[g, ch, 1 - h], dir_r.at[g, ch, 1 - h])
            wait_in(cin.at[g, ch, h], c_r.at[g, ch, h])
            total = (L[g, ch, pos(g, 0), h] + dirt[g, ch, 1 - h]) + cin[g, ch, h]
            for j in range(16):
                if g == 0:
                    S[g, ch, j % 4, h, j // 4] = total[j]
                else:
                    S[g, ch, (j // 4 % 2) * 2 + j // 8, h, j % 4] = total[j]

    def second_send(g, ch):
        o = 1 - g
        if ch in STRAIGHT:
            for j, step in enumerate((2, 1, -1)):
                send(S.at[g, ch, pos(o, step)], qall.at[g, ch, j], qa_s.at[g, ch, j], qa_r.at[g, ch, j], peer(o, step))
            return
        for d, step in DIRS:
            send(S.at[g, ch, pos(o, 2), d], qrel.at[g, ch, d], qrel_s.at[g, ch, d], qrel_r.at[g, ch, d], peer(o, step))
        for d, step in DIRS:
            send(S.at[g, ch, pos(o, step), 1 - d], qdir.at[g, ch, d], qdir_s.at[g, ch, d], qdir_r.at[g, ch, d],
                 peer(o, step))

    def second_combine(g, ch):
        o = 1 - g
        if ch in STRAIGHT:
            return
        for d, step in DIRS:
            wait_in(qrel.at[g, ch, d], qrel_r.at[g, ch, d])
            qrel[g, ch, d] = qrel[g, ch, d] + S[g, ch, pos(o, step), d]
            send(qrel.at[g, ch, d], qin.at[g, ch, d], qc_s.at[g, ch, d], qc_r.at[g, ch, d], peer(o, step))

    def second_sum(g, ch):
        if ch in STRAIGHT:
            for j in range(3):
                wait_in(qall.at[g, ch, j], qa_r.at[g, ch, j])
            total = (S[g, ch, pos(1 - g, 0)] + qall[g, ch, 0]) + (qall[g, ch, 1] + qall[g, ch, 2])
            for h in range(2):
                for j in range(4):
                    T[ch, h, j, g] = total[h, j]
            return
        for h in range(2):
            wait_in(qdir.at[g, ch, 1 - h], qdir_r.at[g, ch, 1 - h])
            wait_in(qin.at[g, ch, h], qc_r.at[g, ch, h])
            total = (S[g, ch, pos(1 - g, 0), h] + qdir[g, ch, 1 - h]) + qin[g, ch, h]
            for j in range(4):
                T[ch, h, j, g] = total[j]

    zsends = []

    def third_send(ch):
        for k in range(4):
            j = lax.rem(z + k, 4)
            zq = core * 4 + j
            for cq in range(2):
                cp = pltpu.make_async_remote_copy(
                    src_ref=T.at[ch, cq, j], dst_ref=zin.at[ch, z], send_sem=z_s.at[ch, j, cq],
                    recv_sem=z_r.at[ch, z], device_id=at(X, zq, y, cq), device_id_type=MESH)
                remote = jnp.logical_or(zq != z, core != cq)
                zsends.append((cp, remote))

                @pl.when(remote)
                def _():
                    cp.start()

                @pl.when(jnp.logical_not(remote))
                def _():
                    zin[ch, z] = T[ch, cq, j]

    def third_sum(ch):
        for k in range(8):
            @pl.when(jnp.logical_or(zhalf != core, k != z))
            def _():
                wait_in(zin.at[ch, k], z_r.at[ch, k])
        total = (zin[ch, 0] + zin[ch, 1]) + (zin[ch, 2] + zin[ch, 3])
        total = total + ((zin[ch, 4] + zin[ch, 5]) + (zin[ch, 6] + zin[ch, 7]))
        out[:, :, ch * CW:(ch + 1) * CW] = total * scale

    def each(fn, ch):
        if 0 <= ch < NCH:
            for g in range(2):
                fn(g, ch)

    pair(0)
    for k in range(NCH + 4):
        pair(k + 1)
        if k < NCH:
            for g in range(2):
                stencil(k, g)
                relay(g, k)
        each(combine, k - 1)
        each(direct, k)
        each(first_sum, k - 2)
        each(second_send, k - 2)
        each(second_combine, k - 3)
        each(second_sum, k - 4)
        if 1 <= k < 5:
            pass_token(k - 1)
        if 0 <= k - 4 < NCH:
            third_send(k - 4)
    for ch in range(NCH):
        third_sum(ch)
    for cp in sends:
        cp.wait_send()
    for cp, remote in zsends:
        @pl.when(remote)
        def _():
            cp.wait_send()


def solution(mesh):
    shots = mesh.shape["shot"] * mesh.shape["tile"]
    scale = 1.0 / float(shots) ** 0.5
    D = pltpu.SemaphoreType.DMA
    V = pltpu.VMEM

    def step(partials):
        return pl.pallas_call(
            functools.partial(kernel, scale),
            out_shape=jax.ShapeDtypeStruct((2, 8, NY), F32),
            in_specs=[pl.BlockSpec(memory_space=pl.ANY)],
            out_specs=pl.BlockSpec(memory_space=pltpu.VMEM),
            scratch_shapes=[
                V((NCH, 8, 2, 18, 8, CW), BF16),
                V((NCH, 8, 2, 18, 8, CW), BF16),
                V((NCH, 8, 2, 18, 8, CW), BF16),
                V((NCH, 10, 2, 144, CW), F32),
                V((2, NCH, 4, 2, 16, 8, CW), F32),
                V((2, NCH, 2, 16, 8, CW), F32),
                V((2, NCH, 2, 16, 8, CW), F32),
                V((2, NCH, 2, 16, 8, CW), F32),
                V((2, NCH, 4, 2, 4, 8, CW), F32),
                V((2, NCH, 2, 4, 8, CW), F32),
                V((2, NCH, 2, 4, 8, CW), F32),
                V((2, NCH, 2, 4, 8, CW), F32),
                V((2, NCH, 3, 2, 4, 8, CW), F32),
                V((NCH, 2, 4, 2, 8, CW), F32),
                V((NCH, 8, 2, 8, CW), F32),
                D((NCH,)), D((NCH,)), D((NCH,)), D((NCH,)),
                D((2, NCH, 2)), D((2, NCH, 2)),
                D((2, NCH, 2)), D((2, NCH, 2)),
                D((2, NCH, 2)), D((2, NCH, 2)),
                D((2, NCH, 2)), D((2, NCH, 2)),
                D((2, NCH, 2)), D((2, NCH, 2)),
                D((2, NCH, 2)), D((2, NCH, 2)),
                D((2, NCH, 3)), D((2, NCH, 3)),
                D((NCH, 4, 2)), D((NCH, 8)),
                pltpu.SemaphoreType.REGULAR((4,)),
            ],
            compiler_params=pltpu.CompilerParams(collective_id=0, has_side_effects=True,
                                                 vmem_limit_bytes=52 * 1024 * 1024),
        )(partials.reshape(8, 64, 8, NY))

    return jax.shard_map(step, mesh=mesh, in_specs=(P(("shot", "tile"), None, None, None),),
                         out_specs=P("shot", "tile", None), check_vma=False)
```

```python
import functools

import jax
import jax.numpy as jnp
from jax import lax
from jax.experimental import pallas as pl
from jax.experimental.pallas import tpu as pltpu
from jax.sharding import PartitionSpec as P

MESH = pl.DeviceIdType.MESH
NY = 512
CW = 128
NT = NY // CW
TILES = (0, 2, 3)
ZTILE = 1
NCH = len(TILES)
UNROLL = 2
STRAIGHT = (2,)
F32 = jnp.float32
BF16 = jnp.bfloat16


def kernel(scale, pin, out, give, mine, theirs, psum, L, rel, dirt, cin, S, qrel, qdir, qin, qall, T, zin, LC, zc, R, xyin,
           give_sem, mine_sem, th_s, th_r, rel_s, rel_r, dir_s, dir_r, c_s, c_r, qrel_s, qrel_r, qdir_s, qdir_r,
           qc_s, qc_r, qa_s, qa_r, z_s, z_r, zc_s, zc_r, xy_s, xy_r, tok):
    s, t = lax.axis_index("shot"), lax.axis_index("tile")
    core, xl = lax.rem(s, 2), s // 2
    xh, z, y = t // 32, lax.rem(t // 4, 8), lax.rem(t, 4)
    X = xh * 2 + xl
    other = 1 - core
    zhalf = z // 4

    def at(Xq, zq, yq, cq):
        return (lax.rem(Xq, 2) * 2 + cq, (Xq // 2) * 32 + zq * 4 + yq)

    def wrap(v, n):
        return lax.rem(v + n, n)

    def pos(g, step):
        return wrap((X if g == 0 else y) + step, 4)

    def peer(g, step):
        return at(pos(0, step), z, y, core) if g == 0 else at(X, z, pos(1, step), core)

    sibling = at(X, z, y, other)

    def load(ch, half, dst, sem):
        cols = pl.ds(ch * CW, CW)
        for q in range(2):
            base = q * 32 + half * 16
            pltpu.make_async_copy(pin.at[:, pl.ds(base, 16), :, cols], dst.at[ch, :, q, pl.ds(1, 16)], sem.at[ch]).start()
            low = jnp.maximum(base - 1, 0)
            pltpu.make_async_copy(pin.at[:, pl.ds(low, 1), :, cols], dst.at[ch, :, q, pl.ds(0, 1)], sem.at[ch]).start()
            high = jnp.minimum(base + 16, 63)
            pltpu.make_async_copy(pin.at[:, pl.ds(high, 1), :, cols], dst.at[ch, :, q, pl.ds(17, 1)], sem.at[ch]).start()

    for ch in range(NT):
        load(ch, other, give, give_sem)
        load(ch, core, mine, mine_sem)

    zring = (at(X, wrap(z + 1, 8), y, core), at(X, wrap(z - 1, 8), y, core))
    barrier = pltpu.get_barrier_semaphore()
    for dev in (sibling, peer(0, 1), peer(0, -1), peer(1, 1), peer(1, -1), *zring):
        pl.semaphore_signal(barrier, inc=1, device_id=dev, device_id_type=MESH)
    for ch in range(NT):
        for q in range(2):
            psum[ch, 0, q] = jnp.zeros((144, CW), F32)
            psum[ch, 9, q] = jnp.zeros((144, CW), F32)
    pl.semaphore_wait(barrier, 7)

    def token(k, devices):
        for dev in devices:
            pl.semaphore_signal(tok.at[k], inc=1, device_id=dev, device_id_type=MESH)

    def pass_token(k):
        pl.semaphore_wait(tok.at[k], 2 if k < 3 else 1)
        if k < 3:
            token(k + 1, zring if k < 2 else (sibling,))

    token(0, zring)

    sends = []

    def send(src, dst, ss, rs, dev):
        cp = pltpu.make_async_remote_copy(src_ref=src, dst_ref=dst, send_sem=ss, recv_sem=rs, device_id=dev,
                                          device_id_type=MESH)
        cp.start()
        sends.append(cp)

    def wait_in(dst, rs):
        pltpu.make_async_copy(dst, dst, rs).wait()

    for ch in range(NT):
        wait_in(give.at[ch], give_sem.at[ch])
        send(give.at[ch], theirs.at[ch], th_s.at[ch], th_r.at[ch], sibling)

    first = jnp.where(core == 0, 0.0, 1.0).astype(F32)
    last = jnp.where(core == 1, 0.0, 1.0).astype(F32)
    lane = lax.broadcasted_iota(jnp.int32, (64, CW), 1)

    def pair(ch):
        wait_in(mine.at[ch], mine_sem.at[ch])
        wait_in(theirs.at[ch], th_r.at[ch])

        @pl.loop(0, 8)
        def _(d):
            for q in range(2):
                psum[ch, d + 1, q] = (mine[ch, d, q].astype(F32) + theirs[ch, d, q].astype(F32)).reshape(144, CW)
            psum[ch, d + 1, 0, 0:8] = psum[ch, d + 1, 0, 0:8] * first
            psum[ch, d + 1, 1, 136:144] = psum[ch, d + 1, 1, 136:144] * last

    def stencil(tile, g):
        ch = TILES.index(tile) if tile != ZTILE else None

        @pl.loop(0, 8, unroll=UNROLL)
        def _(i):
            q, xq = i // 2, lax.rem(i, 2)
            d = 2 * q + g + 1
            for hf in range(2):
                lo = hf * 64 + 8
                mid = slice(lo, lo + 64)
                c = psum[tile, d, xq, mid]
                before = psum[tile - 1, d, xq, mid] if tile > 0 else 0.0
                after = psum[tile + 1, d, xq, mid] if tile < NT - 1 else 0.0
                n = psum[tile, d, xq, slice(lo - 1, lo + 63)] + psum[tile, d, xq, slice(lo + 1, lo + 65)]
                n = n + (psum[tile, d - 1, xq, mid] + psum[tile, d + 1, xq, mid])
                n = n + (pltpu.roll(jnp.where(lane == CW - 1, before, c), 1, 1) +
                         pltpu.roll(jnp.where(lane == 0, after, c), CW - 1, 1))
                r = (6.0 * c - n).reshape(8, 8, CW)
                if tile == ZTILE:
                    for j in range(8):
                        LC[g, hf * 2 + j // 4, lax.rem(q, 2), (q // 2) * 8 + xq * 4 + j % 4] = r[j]
                elif g == 0:
                    L[0, ch, xq * 2 + q // 2, lax.rem(q, 2), pl.ds(hf * 8, 8)] = r
                else:
                    for j in range(8):
                        L[1, ch, j % 4, lax.rem(q, 2), (q // 2) * 8 + xq * 4 + hf * 2 + j // 4] = r[j]

    DIRS = tuple(enumerate((1, -1)))

    def relay(g, ch):
        for d, step in DIRS:
            send(L.at[g, ch, pos(g, 2), d], rel.at[g, ch, d], rel_s.at[g, ch, d], rel_r.at[g, ch, d], peer(g, step))

    def direct(g, ch):
        for d, step in DIRS:
            send(L.at[g, ch, pos(g, step), 1 - d], dirt.at[g, ch, d], dir_s.at[g, ch, d], dir_r.at[g, ch, d],
                 peer(g, step))

    def combine(g, ch):
        for d, step in DIRS:
            wait_in(rel.at[g, ch, d], rel_r.at[g, ch, d])
            rel[g, ch, d] = rel[g, ch, d] + L[g, ch, pos(g, step), d]
            send(rel.at[g, ch, d], cin.at[g, ch, d], c_s.at[g, ch, d], c_r.at[g, ch, d], peer(g, step))

    def first_sum(g, ch):
        for h in range(2):
            wait_in(dirt.at[g, ch, 1 - h], dir_r.at[g, ch, 1 - h])
            wait_in(cin.at[g, ch, h], c_r.at[g, ch, h])
            total = (L[g, ch, pos(g, 0), h] + dirt[g, ch, 1 - h]) + cin[g, ch, h]
            for j in range(16):
                if g == 0:
                    S[g, ch, j % 4, h, j // 4] = total[j]
                else:
                    S[g, ch, (j // 4 % 2) * 2 + j // 8, h, j % 4] = total[j]

    def second_send(g, ch):
        o = 1 - g
        if ch in STRAIGHT:
            for j, step in enumerate((2, 1, -1)):
                send(S.at[g, ch, pos(o, step)], qall.at[g, ch, j], qa_s.at[g, ch, j], qa_r.at[g, ch, j], peer(o, step))
            return
        for d, step in DIRS:
            send(S.at[g, ch, pos(o, 2), d], qrel.at[g, ch, d], qrel_s.at[g, ch, d], qrel_r.at[g, ch, d], peer(o, step))
        for d, step in DIRS:
            send(S.at[g, ch, pos(o, step), 1 - d], qdir.at[g, ch, d], qdir_s.at[g, ch, d], qdir_r.at[g, ch, d],
                 peer(o, step))

    def second_combine(g, ch):
        o = 1 - g
        if ch in STRAIGHT:
            return
        for d, step in DIRS:
            wait_in(qrel.at[g, ch, d], qrel_r.at[g, ch, d])
            qrel[g, ch, d] = qrel[g, ch, d] + S[g, ch, pos(o, step), d]
            send(qrel.at[g, ch, d], qin.at[g, ch, d], qc_s.at[g, ch, d], qc_r.at[g, ch, d], peer(o, step))

    def second_sum(g, ch):
        if ch in STRAIGHT:
            for j in range(3):
                wait_in(qall.at[g, ch, j], qa_r.at[g, ch, j])
            total = (S[g, ch, pos(1 - g, 0)] + qall[g, ch, 0]) + (qall[g, ch, 1] + qall[g, ch, 2])
            for h in range(2):
                for j in range(4):
                    T[ch, h, j, g] = total[h, j]
            return
        for h in range(2):
            wait_in(qdir.at[g, ch, 1 - h], qdir_r.at[g, ch, 1 - h])
            wait_in(qin.at[g, ch, h], qc_r.at[g, ch, h])
            total = (S[g, ch, pos(1 - g, 0), h] + qdir[g, ch, 1 - h]) + qin[g, ch, h]
            for j in range(4):
                T[ch, h, j, g] = total[j]

    zsends = []

    def third_send(ch):
        for k in range(4):
            j = lax.rem(z + k, 4)
            zq = core * 4 + j
            for cq in range(2):
                cp = pltpu.make_async_remote_copy(
                    src_ref=T.at[ch, cq, j], dst_ref=zin.at[ch, z], send_sem=z_s.at[ch, j, cq],
                    recv_sem=z_r.at[ch, z], device_id=at(X, zq, y, cq), device_id_type=MESH)
                remote = jnp.logical_or(zq != z, core != cq)
                zsends.append((cp, remote))

                @pl.when(remote)
                def _():
                    cp.start()

                @pl.when(jnp.logical_not(remote))
                def _():
                    zin[ch, z] = T[ch, cq, j]

    def third_sum(ch):
        for k in range(8):
            @pl.when(jnp.logical_or(zhalf != core, k != z))
            def _():
                wait_in(zin.at[ch, k], z_r.at[ch, k])
        total = (zin[ch, 0] + zin[ch, 1]) + (zin[ch, 2] + zin[ch, 3])
        total = total + ((zin[ch, 4] + zin[ch, 5]) + (zin[ch, 6] + zin[ch, 7]))
        out[:, :, TILES[ch] * CW:(TILES[ch] + 1) * CW] = total * scale

    def send_if(cond, src, dst, ss, rs, dev):
        cp = pltpu.make_async_remote_copy(src_ref=src, dst_ref=dst, send_sem=ss, recv_sem=rs, device_id=dev,
                                          device_id_type=MESH)
        zsends.append((cp, cond))

        @pl.when(cond)
        def _():
            cp.start()

    def z_stage(j):
        for g in range(2):
            for d, step in DIRS:
                dest = wrap(z + step * (5 - j), 8)
                active = dest // 4 == core
                block = lax.rem(dest, 4)
                if j == 1:
                    send_if(active, LC.at[g, block, d], zc.at[d, 0, g, d], zc_s.at[d, 0, g], zc_r.at[d, 0, g], zring[d])
                    continue

                @pl.when(active)
                def _():
                    if j == 2:
                        wait_in(zc.at[d, 0, g, d], zc_r.at[d, 0, g])
                        LC[g, block, d] = LC[g, block, d] + zc[d, 0, g, d]
                    else:
                        wait_in(zc.at[d, j - 2, g], zc_r.at[d, j - 2, g])
                        LC[g, block] = LC[g, block] + zc[d, j - 2, g]

                send_if(active, LC.at[g, block], zc.at[d, j - 1, g], zc_s.at[d, j - 1, g], zc_r.at[d, j - 1, g], zring[d])

    holds = zhalf == core
    me = X * 4 + y

    def z_final():
        block = lax.rem(z, 4)

        @pl.when(holds)
        def _():
            for g in range(2):
                for d in range(2):
                    wait_in(zc.at[d, 3, g], zc_r.at[d, 3, g])

                @pl.loop(0, 16)
                def _(i):
                    for cq in range(2):
                        R[cq, i, g] = (LC[g, block, cq, i] + zc[0, 3, g, cq, i]) + zc[1, 3, g, cq, i]

            xyin[me] = R[core, lax.rem(X, 2) * 8 + (X // 2) * 4 + y]

        for a in (2, 1, 3, 0):
            for b in (2, 1, 3, 0):
                Xq, yq = wrap(X + a, 4), wrap(y + b, 4)
                i = lax.rem(Xq, 2) * 8 + (Xq // 2) * 4 + yq
                for cq in range(2):
                    cond = holds if a or b else jnp.logical_and(holds, core != cq)
                    send_if(cond, R.at[cq, i], xyin.at[me], xy_s.at[a, b, cq], xy_r.at[me], at(Xq, z, yq, cq))

    def xy_sum():
        for k in range(16):
            @pl.when(jnp.logical_or(jnp.logical_not(holds), k != me))
            def _():
                wait_in(xyin.at[k], xy_r.at[k])
        parts = [xyin[k] for k in range(16)]
        while len(parts) > 1:
            parts = [parts[k] + parts[k + 1] for k in range(0, len(parts), 2)]
        out[:, :, ZTILE * CW:(ZTILE + 1) * CW] = parts[0] * scale

    def each(fn, ch):
        for g in range(2):
            fn(g, ch)

    def begin(ch):
        for g in range(2):
            stencil(TILES[ch], g)
            relay(g, ch)

    pair(0)
    pair(1)
    begin(0)
    each(direct, 0)
    pair(2)
    for g in range(2):
        stencil(ZTILE, g)
    z_stage(1)
    pair(3)
    begin(1)
    each(combine, 0)
    each(direct, 1)
    pass_token(0)
    z_stage(2)
    begin(2)
    each(combine, 1)
    each(direct, 2)
    pass_token(1)
    each(first_sum, 0)
    each(second_send, 0)
    z_stage(3)
    each(combine, 2)
    pass_token(2)
    each(first_sum, 1)
    each(second_send, 1)
    each(second_combine, 0)
    z_stage(4)
    each(first_sum, 2)
    each(second_send, 2)
    each(second_combine, 1)
    each(second_sum, 0)
    pass_token(3)
    third_send(0)
    each(second_sum, 1)
    third_send(1)
    z_final()
    each(second_sum, 2)
    third_send(2)
    third_sum(0)
    third_sum(1)
    xy_sum()
    third_sum(2)
    for cp in sends:
        cp.wait_send()
    for cp, remote in zsends:
        @pl.when(remote)
        def _():
            cp.wait_send()


def solution(mesh):
    shots = mesh.shape["shot"] * mesh.shape["tile"]
    scale = 1.0 / float(shots) ** 0.5
    D = pltpu.SemaphoreType.DMA
    V = pltpu.VMEM

    def step(partials):
        return pl.pallas_call(
            functools.partial(kernel, scale),
            out_shape=jax.ShapeDtypeStruct((2, 8, NY), F32),
            in_specs=[pl.BlockSpec(memory_space=pl.ANY)],
            out_specs=pl.BlockSpec(memory_space=pltpu.VMEM),
            scratch_shapes=[
                V((NT, 8, 2, 18, 8, CW), BF16),
                V((NT, 8, 2, 18, 8, CW), BF16),
                V((NT, 8, 2, 18, 8, CW), BF16),
                V((NT, 10, 2, 144, CW), F32),
                V((2, NCH, 4, 2, 16, 8, CW), F32),
                V((2, NCH, 2, 16, 8, CW), F32),
                V((2, NCH, 2, 16, 8, CW), F32),
                V((2, NCH, 2, 16, 8, CW), F32),
                V((2, NCH, 4, 2, 4, 8, CW), F32),
                V((2, NCH, 2, 4, 8, CW), F32),
                V((2, NCH, 2, 4, 8, CW), F32),
                V((2, NCH, 2, 4, 8, CW), F32),
                V((2, NCH, 3, 2, 4, 8, CW), F32),
                V((NCH, 2, 4, 2, 8, CW), F32),
                V((NCH, 8, 2, 8, CW), F32),
                V((2, 4, 2, 16, 8, CW), F32),
                V((2, 4, 2, 2, 16, 8, CW), F32),
                V((2, 16, 2, 8, CW), F32),
                V((16, 2, 8, CW), F32),
                D((NT,)), D((NT,)), D((NT,)), D((NT,)),
                D((2, NCH, 2)), D((2, NCH, 2)),
                D((2, NCH, 2)), D((2, NCH, 2)),
                D((2, NCH, 2)), D((2, NCH, 2)),
                D((2, NCH, 2)), D((2, NCH, 2)),
                D((2, NCH, 2)), D((2, NCH, 2)),
                D((2, NCH, 2)), D((2, NCH, 2)),
                D((2, NCH, 3)), D((2, NCH, 3)),
                D((NCH, 4, 2)), D((NCH, 8)),
                D((2, 4, 2)), D((2, 4, 2)),
                D((4, 4, 2)), D((16,)),
                pltpu.SemaphoreType.REGULAR((4,)),
            ],
            compiler_params=pltpu.CompilerParams(collective_id=0, has_side_effects=True,
                                                 vmem_limit_bytes=52 * 1024 * 1024),
        )(partials.reshape(8, 64, 8, NY))

    return jax.shard_map(step, mesh=mesh, in_specs=(P(("shot", "tile"), None, None, None),),
                         out_specs=P("shot", "tile", None), check_vma=False)
```

```python
import functools

import jax
import jax.numpy as jnp
from jax import lax
from jax.experimental import pallas as pl
from jax.experimental.pallas import tpu as pltpu
from jax.sharding import PartitionSpec as P

MESH = pl.DeviceIdType.MESH
NY = 512
CW = 128
NT = NY // CW
TILES = (0, 2, 3)
ZTILE = 1
NCH = len(TILES)
UNROLL = 2
F32 = jnp.float32
BF16 = jnp.bfloat16


def kernel(scale, pin, out, give, mine, theirs, psum, L, rel, inn, S, qrel, qinn, qall, T, zin, LC, zc, R, xyin,
           give_sem, mine_sem, th_r, rel_r, in_r, qrel_r, qin_r, qall_r, z_r, zc_r, xy_r, snd, zc_s, tok):
    s, t = lax.axis_index("shot"), lax.axis_index("tile")
    core, xl = lax.rem(s, 2), s // 2
    xh, z, y = t // 32, lax.rem(t // 4, 8), lax.rem(t, 4)
    X = xh * 2 + xl
    other = 1 - core
    holds = z // 4 == core
    me = X * 4 + y
    DIRS = tuple(enumerate((1, -1)))

    def at(Xq, zq, yq, cq):
        return (lax.rem(Xq, 2) * 2 + cq, (Xq // 2) * 32 + zq * 4 + yq)

    def wrap(v, n):
        return lax.rem(v + n, n)

    def pos(g, step):
        return wrap((X if g == 0 else y) + step, 4)

    def peer(g, step):
        return at(pos(0, step), z, y, core) if g == 0 else at(X, z, pos(1, step), core)

    sibling = at(X, z, y, other)
    zring = (at(X, wrap(z + 1, 8), y, core), at(X, wrap(z - 1, 8), y, core))
    barrier = pltpu.get_barrier_semaphore()
    for dev in (sibling, peer(0, 1), peer(0, -1), peer(1, 1), peer(1, -1), *zring):
        pl.semaphore_signal(barrier, inc=1, device_id=dev, device_id_type=MESH)

    def load(tile, xq, half, dst, sem):
        cols = pl.ds(tile * CW, CW)
        base = xq * 32 + half * 16
        pltpu.make_async_copy(pin.at[:, pl.ds(base, 16), :, cols], dst.at[tile, xq, :, pl.ds(1, 16)], sem.at[tile, xq]).start()
        low = jnp.maximum(base - 1, 0)
        pltpu.make_async_copy(pin.at[:, pl.ds(low, 1), :, cols], dst.at[tile, xq, :, pl.ds(0, 1)], sem.at[tile, xq]).start()
        high = jnp.minimum(base + 16, 63)
        pltpu.make_async_copy(pin.at[:, pl.ds(high, 1), :, cols], dst.at[tile, xq, :, pl.ds(17, 1)], sem.at[tile, xq]).start()

    far, near = 1 - xh, xh
    ORDER = ((0, far), (1, far), (0, near), (1, near), (2, near), (2, far), (3, near), (3, far))

    def load_both(k):
        for tile, xq in ORDER[k:k + 2]:
            load(tile, xq, other, give, give_sem)
        for tile, xq in ORDER[k:k + 2]:
            load(tile, xq, core, mine, mine_sem)

    load_both(0)
    load_both(2)
    for tile in range(NT):
        for xq in range(2):
            psum[tile, 0, xq] = jnp.zeros((144, CW), F32)
            psum[tile, 9, xq] = jnp.zeros((144, CW), F32)
    pl.semaphore_wait(barrier, 7)

    def token(k, devices):
        for dev in devices:
            pl.semaphore_signal(tok.at[k], inc=1, device_id=dev, device_id_type=MESH)

    def pass_token(k):
        pl.semaphore_wait(tok.at[k], 2 if k < 3 else 1)
        if k < 3:
            token(k + 1, zring if k < 2 else (sibling,))

    def remote(src, dst, ss, rs, dev):
        return pltpu.make_async_remote_copy(src_ref=src, dst_ref=dst, send_sem=ss, recv_sem=rs, device_id=dev,
                                            device_id_type=MESH)

    def send(src, dst, ss, rs, dev):
        remote(src, dst, ss, rs, dev).start()

    def send_if(cond, src, dst, ss, rs, dev):
        @pl.when(cond)
        def _():
            remote(src, dst, ss, rs, dev).start()

    def wait_in(dst, rs):
        pltpu.make_async_copy(dst, dst, rs).wait()

    def hand_over(k):
        for tile, xq in ORDER[k:k + 2]:
            wait_in(give.at[tile, xq], give_sem.at[tile, xq])
            send(give.at[tile, xq], theirs.at[tile, xq], snd.at[0], th_r.at[tile, xq], sibling)

    hand_over(0)
    hand_over(2)
    load_both(4)
    load_both(6)
    token(0, zring)

    lane = lax.broadcasted_iota(jnp.int32, (64, CW), 1)

    def pair(k):
        for tile, xq in ORDER[k:k + 2]:
            wait_in(mine.at[tile, xq], mine_sem.at[tile, xq])
            wait_in(theirs.at[tile, xq], th_r.at[tile, xq])
            low = jnp.where(jnp.logical_and(core == 0, xq == 0), 0.0, 1.0).astype(F32)
            high = jnp.where(jnp.logical_and(core == 1, xq == 1), 0.0, 1.0).astype(F32)

            @pl.loop(0, 8)
            def _(d):
                v = (mine[tile, xq, d].astype(F32) + theirs[tile, xq, d].astype(F32)).reshape(144, CW)
                psum[tile, d + 1, xq, 8:136] = v[8:136]
                psum[tile, d + 1, xq, 0:8] = v[0:8] * low
                psum[tile, d + 1, xq, 136:144] = v[136:144] * high

    def stencil(tile, g, xq):
        ch = TILES.index(tile) if tile != ZTILE else None

        @pl.loop(0, 4, unroll=UNROLL)
        def _(q):
            d = 2 * q + g + 1
            for hf in range(2):
                lo = hf * 64 + 8
                mid = slice(lo, lo + 64)
                c = psum[tile, d, xq, mid]
                before = psum[tile - 1, d, xq, mid] if tile > 0 else 0.0
                after = psum[tile + 1, d, xq, mid] if tile < NT - 1 else 0.0
                n = psum[tile, d, xq, slice(lo - 1, lo + 63)] + psum[tile, d, xq, slice(lo + 1, lo + 65)]
                n = n + (psum[tile, d - 1, xq, mid] + psum[tile, d + 1, xq, mid])
                n = n + (pltpu.roll(jnp.where(lane == CW - 1, before, c), 1, 1) +
                         pltpu.roll(jnp.where(lane == 0, after, c), CW - 1, 1))
                r = (6.0 * c - n).reshape(8, 8, CW)
                if tile == ZTILE:
                    for j in range(8):
                        LC[g, hf * 2 + j // 4, lax.rem(q, 2), (q // 2) * 8 + xq * 4 + j % 4] = r[j]
                elif g == 0:
                    L[0, ch, xq * 2 + q // 2, lax.rem(q, 2), pl.ds(hf * 8, 8)] = r
                else:
                    for j in range(8):
                        L[1, ch, j % 4, lax.rem(q, 2), (q // 2) * 8 + xq * 4 + hf * 2 + j // 4] = r[j]

    def relay(g, ch):
        for d, step in DIRS:
            send(L.at[g, ch, pos(g, 2), d], rel.at[g, ch, d], snd.at[1], rel_r.at[g, ch], peer(g, step))

    def direct(g, ch):
        for d, step in DIRS:
            send(L.at[g, ch, pos(g, step), 1 - d], inn.at[g, ch, 0, d], snd.at[2], in_r.at[g, ch], peer(g, step))

    def combine(g, ch):
        wait_in(rel.at[g, ch], rel_r.at[g, ch])
        for d, step in DIRS:
            rel[g, ch, d] = rel[g, ch, d] + L[g, ch, pos(g, step), d]
            send(rel.at[g, ch, d], inn.at[g, ch, 1, d], snd.at[2], in_r.at[g, ch], peer(g, step))

    def first_sum(g, ch):
        wait_in(inn.at[g, ch], in_r.at[g, ch])
        for h in range(2):
            total = (L[g, ch, pos(g, 0), h] + inn[g, ch, 0, 1 - h]) + inn[g, ch, 1, h]
            for j in range(16):
                if g == 0:
                    S[g, ch, j % 4, h, j // 4] = total[j]
                else:
                    S[g, ch, (j // 4 % 2) * 2 + j // 8, h, j % 4] = total[j]

    def second_send(g, ch):
        o = 1 - g
        if ch == NCH - 1:
            for j, step in enumerate((2, 1, -1)):
                send(S.at[g, ch, pos(o, step)], qall.at[g, j], snd.at[5], qall_r.at[g], peer(o, step))
            return
        for d, step in DIRS:
            send(S.at[g, ch, pos(o, 2), d], qrel.at[g, ch, d], snd.at[3], qrel_r.at[g, ch], peer(o, step))
        for d, step in DIRS:
            send(S.at[g, ch, pos(o, step), 1 - d], qinn.at[g, ch, 0, d], snd.at[4], qin_r.at[g, ch], peer(o, step))

    def second_combine(g, ch):
        o = 1 - g
        wait_in(qrel.at[g, ch], qrel_r.at[g, ch])
        for d, step in DIRS:
            qrel[g, ch, d] = qrel[g, ch, d] + S[g, ch, pos(o, step), d]
            send(qrel.at[g, ch, d], qinn.at[g, ch, 1, d], snd.at[4], qin_r.at[g, ch], peer(o, step))

    def second_sum(g, ch):
        own = S[g, ch, pos(1 - g, 0)]
        if ch == NCH - 1:
            wait_in(qall.at[g], qall_r.at[g])
            total = (own + qall[g, 0]) + (qall[g, 1] + qall[g, 2])
            for h in range(2):
                for j in range(4):
                    T[ch, h, j, g] = total[h, j]
            return
        wait_in(qinn.at[g, ch], qin_r.at[g, ch])
        for h in range(2):
            total = (own[h] + qinn[g, ch, 0, 1 - h]) + qinn[g, ch, 1, h]
            for j in range(4):
                T[ch, h, j, g] = total[j]

    def third_send(ch):
        for k in (2, 1, 3, 0):
            j = lax.rem(z + k, 4)
            zq = core * 4 + j
            for cq in range(2):
                send_if(jnp.logical_or(zq != z, core != cq), T.at[ch, cq, j], zin.at[ch, z], snd.at[6], z_r.at[ch],
                        at(X, zq, y, cq))

        @pl.when(holds)
        def _():
            zin[ch, z] = T[ch, core, lax.rem(z, 4)]

    def third_sum(ch):
        @pl.when(holds)
        def _():
            wait_in(zin.at[ch, pl.ds(0, 7)], z_r.at[ch])

        @pl.when(jnp.logical_not(holds))
        def _():
            wait_in(zin.at[ch], z_r.at[ch])

        total = (zin[ch, 0] + zin[ch, 1]) + (zin[ch, 2] + zin[ch, 3])
        total = total + ((zin[ch, 4] + zin[ch, 5]) + (zin[ch, 6] + zin[ch, 7]))
        out[:, :, TILES[ch] * CW:(TILES[ch] + 1) * CW] = total * scale

    def z_active(j, step):
        dest = wrap(z + step * (5 - j), 8)
        return dest // 4 == core, lax.rem(dest, 4)

    def z_stage(j):
        for g in range(2):
            for d, step in DIRS:
                active, block = z_active(j, step)
                if j == 1:
                    send_if(active, LC.at[g, block, d], zc.at[d, 0, g, d], zc_s.at[d, 0], zc_r.at[d, 0, g], zring[d])
                    continue

                @pl.when(active)
                def _():
                    if j == 2:
                        wait_in(zc.at[d, 0, g, d], zc_r.at[d, 0, g])
                        LC[g, block, d] = LC[g, block, d] + zc[d, 0, g, d]
                    else:
                        wait_in(zc.at[d, j - 2, g], zc_r.at[d, j - 2, g])
                        LC[g, block] = LC[g, block] + zc[d, j - 2, g]
                    send(LC.at[g, block], zc.at[d, j - 1, g], zc_s.at[d, j - 1], zc_r.at[d, j - 1, g], zring[d])

    def z_final():
        block = lax.rem(z, 4)

        @pl.when(holds)
        def _():
            for g in range(2):
                for d in range(2):
                    wait_in(zc.at[d, 3, g], zc_r.at[d, 3, g])

                @pl.loop(0, 16)
                def _(i):
                    for cq in range(2):
                        R[cq * 16 + i, g] = (LC[g, block, cq, i] + zc[0, 3, g, cq, i]) + zc[1, 3, g, cq, i]

            xyin[me] = R[core * 16 + lax.rem(X, 2) * 8 + (X // 2) * 4 + y]
            for a in (2, 1, 3, 0):
                for b in (2, 1, 3, 0):
                    Xq, yq = wrap(X + a, 4), wrap(y + b, 4)
                    i = lax.rem(Xq, 2) * 8 + (Xq // 2) * 4 + yq
                    for cq in range(2):
                        if a or b:
                            send(R.at[cq * 16 + i], xyin.at[me], snd.at[7], xy_r, at(Xq, z, yq, cq))
                        else:
                            send_if(core != cq, R.at[cq * 16 + i], xyin.at[me], snd.at[7], xy_r, at(Xq, z, yq, cq))

    def xy_sum():
        @pl.when(holds)
        def _():
            wait_in(xyin.at[pl.ds(0, 15)], xy_r)

        @pl.when(jnp.logical_not(holds))
        def _():
            wait_in(xyin, xy_r)

        parts = [xyin[k] for k in range(16)]
        while len(parts) > 1:
            parts = [parts[k] + parts[k + 1] for k in range(0, len(parts), 2)]
        out[:, :, ZTILE * CW:(ZTILE + 1) * CW] = parts[0] * scale

    def each(fn, ch):
        for g in range(2):
            fn(g, ch)

    def begin(ch):
        for g in range(2):
            for xq in range(2):
                stencil(TILES[ch], g, xq)
            relay(g, ch)

    pair(0)
    stencil(0, 0, far)
    relay(0, 0)
    pair(2)
    hand_over(4)
    stencil(0, 1, far)
    stencil(0, 1, near)
    relay(1, 0)
    direct(1, 0)
    stencil(0, 0, near)
    direct(0, 0)
    hand_over(6)
    pair(4)
    for g in range(2):
        for xq in range(2):
            stencil(ZTILE, g, xq)
    z_stage(1)
    pair(6)
    begin(1)
    each(combine, 0)
    each(direct, 1)
    pass_token(0)
    z_stage(2)
    begin(2)
    each(combine, 1)
    each(direct, 2)
    pass_token(1)
    each(first_sum, 0)
    each(second_send, 0)
    z_stage(3)
    each(combine, 2)
    pass_token(2)
    each(first_sum, 1)
    each(second_send, 1)
    each(second_combine, 0)
    z_stage(4)
    each(first_sum, 2)
    each(second_send, 2)
    each(second_combine, 1)
    each(second_sum, 0)
    pass_token(3)
    third_send(0)
    z_final()
    each(second_sum, 1)
    third_send(1)
    each(second_sum, 2)
    third_send(2)
    third_sum(0)
    third_sum(1)
    xy_sum()
    third_sum(2)
    for k, buffer in enumerate((theirs, rel, inn, qrel, qinn, qall)):
        wait_in(buffer, snd.at[k])

    @pl.when(holds)
    def _():
        wait_in(zin.at[:, pl.ds(0, 7)], snd.at[6])
        wait_in(R.at[pl.ds(0, 31)], snd.at[7])

    @pl.when(jnp.logical_not(holds))
    def _():
        wait_in(zin, snd.at[6])

    for j in range(1, 5):
        for d, step in DIRS:
            @pl.when(z_active(j, step)[0])
            def _():
                sent = zc.at[d, 0, 0] if j == 1 else zc.at[d, j - 1]
                wait_in(sent, zc_s.at[d, j - 1])


def solution(mesh):
    shots = mesh.shape["shot"] * mesh.shape["tile"]
    scale = 1.0 / float(shots) ** 0.5
    D = pltpu.SemaphoreType.DMA
    V = pltpu.VMEM

    def step(partials):
        return pl.pallas_call(
            functools.partial(kernel, scale),
            out_shape=jax.ShapeDtypeStruct((2, 8, NY), F32),
            in_specs=[pl.BlockSpec(memory_space=pl.ANY)],
            out_specs=pl.BlockSpec(memory_space=pltpu.VMEM),
            scratch_shapes=[
                V((NT, 2, 8, 18, 8, CW), BF16),
                V((NT, 2, 8, 18, 8, CW), BF16),
                V((NT, 2, 8, 18, 8, CW), BF16),
                V((NT, 10, 2, 144, CW), F32),
                V((2, NCH, 4, 2, 16, 8, CW), F32),
                V((2, NCH, 2, 16, 8, CW), F32),
                V((2, NCH, 2, 2, 16, 8, CW), F32),
                V((2, NCH, 4, 2, 4, 8, CW), F32),
                V((2, NCH - 1, 2, 4, 8, CW), F32),
                V((2, NCH - 1, 2, 2, 4, 8, CW), F32),
                V((2, 3, 2, 4, 8, CW), F32),
                V((NCH, 2, 4, 2, 8, CW), F32),
                V((NCH, 8, 2, 8, CW), F32),
                V((2, 4, 2, 16, 8, CW), F32),
                V((2, 4, 2, 2, 16, 8, CW), F32),
                V((32, 2, 8, CW), F32),
                V((16, 2, 8, CW), F32),
                D((NT, 2)), D((NT, 2)), D((NT, 2)),
                D((2, NCH)), D((2, NCH)),
                D((2, NCH - 1)), D((2, NCH - 1)), D((2,)),
                D((NCH,)), D((2, 4, 2)), D(()),
                D((8,)), D((2, 4)),
                pltpu.SemaphoreType.REGULAR((4,)),
            ],
            compiler_params=pltpu.CompilerParams(collective_id=0, has_side_effects=True,
                                                 vmem_limit_bytes=52 * 1024 * 1024),
        )(partials.reshape(8, 64, 8, NY))

    return jax.shard_map(step, mesh=mesh, in_specs=(P(("shot", "tile"), None, None, None),),
                         out_specs=P("shot", "tile", None), check_vma=False)
```

```python
import functools

import jax
import jax.numpy as jnp
from jax import lax
from jax.experimental import pallas as pl
from jax.experimental.pallas import tpu as pltpu
from jax.sharding import PartitionSpec as P

MESH = pl.DeviceIdType.MESH
NY = 512
CW = 128
NT = NY // CW
TILES = (0, 1, 3)
ZTILE = 2
NCH = len(TILES)
UNROLL = 4
F32 = jnp.float32
BF16 = jnp.bfloat16


def kernel(scale, pin, out, give, mine, theirs, psum, L, rel, inn, S, qrel, qinn, qall, T, zin, LC, zc, R, xyin,
           give_sem, mine_sem, th_r, rel_r, in_r, qrel_r, qin_r, qall_r, z_r, zc_r, xy_r, snd, zc_s, tok):
    s, t = lax.axis_index("shot"), lax.axis_index("tile")
    core, xl = lax.rem(s, 2), s // 2
    xh, z, y = t // 32, lax.rem(t // 4, 8), lax.rem(t, 4)
    X = xh * 2 + xl
    other = 1 - core
    holds = z // 4 == core
    me = X * 4 + y
    DIRS = tuple(enumerate((1, -1)))

    def at(Xq, zq, yq, cq):
        return (lax.rem(Xq, 2) * 2 + cq, (Xq // 2) * 32 + zq * 4 + yq)

    def wrap(v, n):
        return lax.rem(v + n, n)

    def pos(g, step):
        return wrap((X if g == 0 else y) + step, 4)

    def peer(g, step):
        return at(pos(0, step), z, y, core) if g == 0 else at(X, z, pos(1, step), core)

    sibling = at(X, z, y, other)
    zring = (at(X, wrap(z + 1, 8), y, core), at(X, wrap(z - 1, 8), y, core))
    barrier = pltpu.get_barrier_semaphore()
    for dev in (sibling, peer(0, 1), peer(0, -1), peer(1, 1), peer(1, -1), *zring):
        pl.semaphore_signal(barrier, inc=1, device_id=dev, device_id_type=MESH)

    def load(tile, xq, half, dst, sem):
        cols = pl.ds(tile * CW, CW)
        base = xq * 32 + half * 16
        pltpu.make_async_copy(pin.at[:, pl.ds(base, 16), :, cols], dst.at[tile, xq, :, pl.ds(1, 16)], sem.at[tile, xq]).start()
        low = jnp.maximum(base - 1, 0)
        pltpu.make_async_copy(pin.at[:, pl.ds(low, 1), :, cols], dst.at[tile, xq, :, pl.ds(0, 1)], sem.at[tile, xq]).start()
        high = jnp.minimum(base + 16, 63)
        pltpu.make_async_copy(pin.at[:, pl.ds(high, 1), :, cols], dst.at[tile, xq, :, pl.ds(17, 1)], sem.at[tile, xq]).start()

    far, near = 1 - xh, xh
    ORDER = ((0, far), (1, far), (0, near), (1, near), (2, near), (2, far), (3, near), (3, far))

    def load_both(k):
        for tile, xq in ORDER[k:k + 2]:
            load(tile, xq, other, give, give_sem)
        for tile, xq in ORDER[k:k + 2]:
            load(tile, xq, core, mine, mine_sem)

    load_both(0)
    load_both(2)
    for tile in range(NT):
        for xq in range(2):
            psum[tile, 0, xq] = jnp.zeros((144, CW), F32)
            psum[tile, 9, xq] = jnp.zeros((144, CW), F32)
    pl.semaphore_wait(barrier, 7)

    def token(k, devices):
        for dev in devices:
            pl.semaphore_signal(tok.at[k], inc=1, device_id=dev, device_id_type=MESH)

    def pass_token(k):
        pl.semaphore_wait(tok.at[k], 2 if k < 3 else 1)
        if k < 3:
            token(k + 1, zring if k < 2 else (sibling,))

    def remote(src, dst, ss, rs, dev):
        return pltpu.make_async_remote_copy(src_ref=src, dst_ref=dst, send_sem=ss, recv_sem=rs, device_id=dev,
                                            device_id_type=MESH)

    def send(src, dst, ss, rs, dev):
        remote(src, dst, ss, rs, dev).start()

    def send_if(cond, src, dst, ss, rs, dev):
        @pl.when(cond)
        def _():
            remote(src, dst, ss, rs, dev).start()

    def wait_in(dst, rs):
        pltpu.make_async_copy(dst, dst, rs).wait()

    def hand_over(k):
        for tile, xq in ORDER[k:k + 2]:
            wait_in(give.at[tile, xq], give_sem.at[tile, xq])
            send(give.at[tile, xq], theirs.at[tile, xq], snd.at[0], th_r.at[tile, xq], sibling)

    hand_over(0)
    load_both(4)
    hand_over(2)
    load_both(6)
    token(0, zring)

    lane = lax.broadcasted_iota(jnp.int32, (64, CW), 1)

    def pair(k):
        for tile, xq in ORDER[k:k + 2]:
            wait_in(mine.at[tile, xq], mine_sem.at[tile, xq])
            wait_in(theirs.at[tile, xq], th_r.at[tile, xq])
            low = jnp.where(jnp.logical_and(core == 0, xq == 0), 0.0, 1.0).astype(F32)
            high = jnp.where(jnp.logical_and(core == 1, xq == 1), 0.0, 1.0).astype(F32)

            @pl.loop(0, 8, unroll=4)
            def _(d):
                v = (mine[tile, xq, d].astype(F32) + theirs[tile, xq, d].astype(F32)).reshape(144, CW)
                psum[tile, d + 1, xq, 8:136] = v[8:136]
                psum[tile, d + 1, xq, 0:8] = v[0:8] * low
                psum[tile, d + 1, xq, 136:144] = v[136:144] * high

    def stencil(tile, g, xq):
        ch = TILES.index(tile) if tile != ZTILE else None

        @pl.loop(0, 4, unroll=UNROLL)
        def _(q):
            d = 2 * q + g + 1
            for hf in range(2):
                lo = hf * 64 + 8
                mid = slice(lo, lo + 64)
                c = psum[tile, d, xq, mid]
                before = psum[tile - 1, d, xq, mid] if tile > 0 else 0.0
                after = psum[tile + 1, d, xq, mid] if tile < NT - 1 else 0.0
                n = psum[tile, d, xq, slice(lo - 1, lo + 63)] + psum[tile, d, xq, slice(lo + 1, lo + 65)]
                n = n + (psum[tile, d - 1, xq, mid] + psum[tile, d + 1, xq, mid])
                n = n + (pltpu.roll(jnp.where(lane == CW - 1, before, c), 1, 1) +
                         pltpu.roll(jnp.where(lane == 0, after, c), CW - 1, 1))
                r = (6.0 * c - n).reshape(8, 8, CW)
                if tile == ZTILE:
                    for j in range(8):
                        LC[g, hf * 2 + j // 4, lax.rem(q, 2), (q // 2) * 8 + xq * 4 + j % 4] = r[j]
                elif g == 0:
                    L[0, ch, xq * 2 + q // 2, lax.rem(q, 2), pl.ds(hf * 8, 8)] = r
                else:
                    for j in range(8):
                        L[1, ch, j % 4, lax.rem(q, 2), (q // 2) * 8 + xq * 4 + hf * 2 + j // 4] = r[j]

    def relay(g, ch):
        for d, step in DIRS:
            send(L.at[g, ch, pos(g, 2), d], rel.at[g, ch, d], snd.at[1], rel_r.at[g, ch], peer(g, step))

    def direct(g, ch):
        for d, step in DIRS:
            send(L.at[g, ch, pos(g, step), 1 - d], inn.at[g, ch, 0, d], snd.at[2], in_r.at[g, ch], peer(g, step))

    def combine(g, ch):
        wait_in(rel.at[g, ch], rel_r.at[g, ch])
        for d, step in DIRS:
            rel[g, ch, d] = rel[g, ch, d] + L[g, ch, pos(g, step), d]
            send(rel.at[g, ch, d], inn.at[g, ch, 1, d], snd.at[2], in_r.at[g, ch], peer(g, step))

    def first_sum(g, ch):
        wait_in(inn.at[g, ch], in_r.at[g, ch])
        for h in range(2):
            total = (L[g, ch, pos(g, 0), h] + inn[g, ch, 0, 1 - h]) + inn[g, ch, 1, h]
            for j in range(16):
                if g == 0:
                    S[g, ch, j % 4, h, j // 4] = total[j]
                else:
                    S[g, ch, (j // 4 % 2) * 2 + j // 8, h, j % 4] = total[j]

    def second_send(g, ch):
        o = 1 - g
        if ch == NCH - 1:
            for j, step in enumerate((2, 1, -1)):
                send(S.at[g, ch, pos(o, step)], qall.at[g, j], snd.at[5], qall_r.at[g], peer(o, step))
            return
        for d, step in DIRS:
            send(S.at[g, ch, pos(o, 2), d], qrel.at[g, ch, d], snd.at[3], qrel_r.at[g, ch], peer(o, step))
        for d, step in DIRS:
            send(S.at[g, ch, pos(o, step), 1 - d], qinn.at[g, ch, 0, d], snd.at[4], qin_r.at[g, ch], peer(o, step))

    def second_combine(g, ch):
        o = 1 - g
        wait_in(qrel.at[g, ch], qrel_r.at[g, ch])
        for d, step in DIRS:
            qrel[g, ch, d] = qrel[g, ch, d] + S[g, ch, pos(o, step), d]
            send(qrel.at[g, ch, d], qinn.at[g, ch, 1, d], snd.at[4], qin_r.at[g, ch], peer(o, step))

    def second_sum(g, ch):
        own = S[g, ch, pos(1 - g, 0)]
        if ch == NCH - 1:
            wait_in(qall.at[g], qall_r.at[g])
            total = (own + qall[g, 0]) + (qall[g, 1] + qall[g, 2])
            for h in range(2):
                for j in range(4):
                    T[ch, h, j, g] = total[h, j]
            return
        wait_in(qinn.at[g, ch], qin_r.at[g, ch])
        for h in range(2):
            total = (own[h] + qinn[g, ch, 0, 1 - h]) + qinn[g, ch, 1, h]
            for j in range(4):
                T[ch, h, j, g] = total[j]

    def third_send(ch):
        for k in (2, 1, 3, 0):
            j = lax.rem(z + k, 4)
            zq = core * 4 + j
            for cq in range(2):
                send_if(jnp.logical_or(zq != z, core != cq), T.at[ch, cq, j], zin.at[ch, z], snd.at[6], z_r.at[ch],
                        at(X, zq, y, cq))

        @pl.when(holds)
        def _():
            zin[ch, z] = T[ch, core, lax.rem(z, 4)]

    def third_sum(ch):
        @pl.when(holds)
        def _():
            wait_in(zin.at[ch, pl.ds(0, 7)], z_r.at[ch])

        @pl.when(jnp.logical_not(holds))
        def _():
            wait_in(zin.at[ch], z_r.at[ch])

        total = (zin[ch, 0] + zin[ch, 1]) + (zin[ch, 2] + zin[ch, 3])
        total = total + ((zin[ch, 4] + zin[ch, 5]) + (zin[ch, 6] + zin[ch, 7]))
        out[:, :, TILES[ch] * CW:(TILES[ch] + 1) * CW] = total * scale

    def z_active(j, step):
        dest = wrap(z + step * (5 - j), 8)
        return dest // 4 == core, lax.rem(dest, 4)

    def z_part(j, short):
        for g in range(2):
            for d, step in DIRS:
                active, block = z_active(j, step)
                cq = 1 - d if short else d

                @pl.when(active)
                def _():
                    if j > 1 + short:
                        wait_in(zc.at[d, j - 2, g, cq], zc_r.at[d, j - 2, g, cq])
                        LC[g, block, cq] = LC[g, block, cq] + zc[d, j - 2, g, cq]
                    send(LC.at[g, block, cq], zc.at[d, j - 1, g, cq], zc_s.at[d, j - 1], zc_r.at[d, j - 1, g, cq], zring[d])

    def z_final():
        block = lax.rem(z, 4)

        @pl.when(holds)
        def _():
            for g in range(2):
                for d in range(2):
                    for cq in range(2):
                        wait_in(zc.at[d, 3, g, cq], zc_r.at[d, 3, g, cq])

                @pl.loop(0, 16)
                def _(i):
                    for cq in range(2):
                        R[cq * 16 + i, g] = (LC[g, block, cq, i] + zc[0, 3, g, cq, i]) + zc[1, 3, g, cq, i]

            xyin[me] = R[core * 16 + lax.rem(X, 2) * 8 + (X // 2) * 4 + y]
            for a in (2, 1, 3, 0):
                for b in (2, 1, 3, 0):
                    Xq, yq = wrap(X + a, 4), wrap(y + b, 4)
                    i = lax.rem(Xq, 2) * 8 + (Xq // 2) * 4 + yq
                    for cq in range(2):
                        if a or b:
                            send(R.at[cq * 16 + i], xyin.at[me], snd.at[7], xy_r, at(Xq, z, yq, cq))
                        else:
                            send_if(core != cq, R.at[cq * 16 + i], xyin.at[me], snd.at[7], xy_r, at(Xq, z, yq, cq))

    def xy_sum():
        @pl.when(holds)
        def _():
            wait_in(xyin.at[pl.ds(0, 15)], xy_r)

        @pl.when(jnp.logical_not(holds))
        def _():
            wait_in(xyin, xy_r)

        parts = [xyin[k] for k in range(16)]
        while len(parts) > 1:
            parts = [parts[k] + parts[k + 1] for k in range(0, len(parts), 2)]
        out[:, :, ZTILE * CW:(ZTILE + 1) * CW] = parts[0] * scale

    def each(fn, ch):
        for g in range(2):
            fn(g, ch)

    def begin(ch):
        for g in range(2):
            for xq in range(2):
                stencil(TILES[ch], g, xq)
            relay(g, ch)

    pair(0)
    stencil(0, 0, far)
    relay(0, 0)
    hand_over(4)
    stencil(0, 1, far)
    pair(2)
    stencil(0, 1, near)
    relay(1, 0)
    direct(1, 0)
    stencil(0, 0, near)
    direct(0, 0)
    hand_over(6)
    pair(4)
    begin(1)
    combine(0, 0)
    direct(0, 1)
    pair(6)
    stencil(ZTILE, 0, 0)
    stencil(ZTILE, 0, 1)
    combine(1, 0)
    direct(1, 1)
    stencil(ZTILE, 1, 0)
    stencil(ZTILE, 1, 1)
    z_part(1, 0)
    pass_token(0)
    begin(2)
    z_part(2, 1)
    each(combine, 1)
    each(direct, 2)
    z_part(2, 0)
    pass_token(1)
    each(first_sum, 0)
    each(second_send, 0)
    z_part(3, 1)
    each(combine, 2)
    z_part(3, 0)
    pass_token(2)
    each(first_sum, 1)
    each(second_send, 1)
    z_part(4, 1)
    each(second_combine, 0)
    z_part(4, 0)
    each(second_combine, 1)
    each(first_sum, 2)
    each(second_send, 2)
    each(second_sum, 0)
    pass_token(3)
    third_send(0)
    z_final()
    each(second_sum, 1)
    third_send(1)
    each(second_sum, 2)
    third_send(2)
    third_sum(0)
    third_sum(1)
    xy_sum()
    third_sum(2)
    for k, buffer in enumerate((theirs, rel, inn, qrel, qinn, qall)):
        wait_in(buffer, snd.at[k])

    @pl.when(holds)
    def _():
        wait_in(zin.at[:, pl.ds(0, 7)], snd.at[6])
        wait_in(R.at[pl.ds(0, 31)], snd.at[7])

    @pl.when(jnp.logical_not(holds))
    def _():
        wait_in(zin, snd.at[6])

    for j in range(1, 5):
        for d, step in DIRS:
            @pl.when(z_active(j, step)[0])
            def _():
                sent = zc.at[d, 0, 0] if j == 1 else zc.at[d, j - 1]
                wait_in(sent, zc_s.at[d, j - 1])


def solution(mesh):
    shots = mesh.shape["shot"] * mesh.shape["tile"]
    scale = 1.0 / float(shots) ** 0.5
    D = pltpu.SemaphoreType.DMA
    V = pltpu.VMEM

    def step(partials):
        return pl.pallas_call(
            functools.partial(kernel, scale),
            out_shape=jax.ShapeDtypeStruct((2, 8, NY), F32),
            in_specs=[pl.BlockSpec(memory_space=pl.ANY)],
            out_specs=pl.BlockSpec(memory_space=pltpu.VMEM),
            scratch_shapes=[
                V((NT, 2, 8, 18, 8, CW), BF16),
                V((NT, 2, 8, 18, 8, CW), BF16),
                V((NT, 2, 8, 18, 8, CW), BF16),
                V((NT, 10, 2, 144, CW), F32),
                V((2, NCH, 4, 2, 16, 8, CW), F32),
                V((2, NCH, 2, 16, 8, CW), F32),
                V((2, NCH, 2, 2, 16, 8, CW), F32),
                V((2, NCH, 4, 2, 4, 8, CW), F32),
                V((2, NCH - 1, 2, 4, 8, CW), F32),
                V((2, NCH - 1, 2, 2, 4, 8, CW), F32),
                V((2, 3, 2, 4, 8, CW), F32),
                V((NCH, 2, 4, 2, 8, CW), F32),
                V((NCH, 8, 2, 8, CW), F32),
                V((2, 4, 2, 16, 8, CW), F32),
                V((2, 4, 2, 2, 16, 8, CW), F32),
                V((32, 2, 8, CW), F32),
                V((16, 2, 8, CW), F32),
                D((NT, 2)), D((NT, 2)), D((NT, 2)),
                D((2, NCH)), D((2, NCH)),
                D((2, NCH - 1)), D((2, NCH - 1)), D((2,)),
                D((NCH,)), D((2, 4, 2, 2)), D(()),
                D((8,)), D((2, 4)),
                pltpu.SemaphoreType.REGULAR((4,)),
            ],
            compiler_params=pltpu.CompilerParams(collective_id=0, has_side_effects=True,
                                                 vmem_limit_bytes=52 * 1024 * 1024),
        )(partials.reshape(8, 64, 8, NY))

    return jax.shard_map(step, mesh=mesh, in_specs=(P(("shot", "tile"), None, None, None),),
                         out_specs=P("shot", "tile", None), check_vma=False)
```

```python
import functools

import jax
import jax.numpy as jnp
from jax import lax
from jax.experimental import pallas as pl
from jax.experimental.pallas import tpu as pltpu
from jax.sharding import PartitionSpec as P

MESH = pl.DeviceIdType.MESH
NY = 512
CW = 128
NT = NY // CW
TILES = (0, 2, 3)
ZTILE = 1
NCH = len(TILES)
UNROLL = 4
F32 = jnp.float32
BF16 = jnp.bfloat16


def kernel(scale, pin, out, give, mine, theirs, psum, L, rel, inn, S, qrel, qinn, qall, T, zin, LC, zc, R, xyin,
           give_sem, mine_sem, th_r, rel_r, in_r, qrel_r, qin_r, qall_r, z_r, zc_r, xy_r, snd, zc_s, tok):
    s, t = lax.axis_index("shot"), lax.axis_index("tile")
    core, xl = lax.rem(s, 2), s // 2
    xh, z, y = t // 32, lax.rem(t // 4, 8), lax.rem(t, 4)
    X = xh * 2 + xl
    other = 1 - core
    holds = z // 4 == core
    me = X * 4 + y
    DIRS = tuple(enumerate((1, -1)))

    def at(Xq, zq, yq, cq):
        return (lax.rem(Xq, 2) * 2 + cq, (Xq // 2) * 32 + zq * 4 + yq)

    def wrap(v, n):
        return lax.rem(v + n, n)

    def pos(g, step):
        return wrap((X if g == 0 else y) + step, 4)

    def peer(g, step):
        return at(pos(0, step), z, y, core) if g == 0 else at(X, z, pos(1, step), core)

    sibling = at(X, z, y, other)
    zring = (at(X, wrap(z + 1, 8), y, core), at(X, wrap(z - 1, 8), y, core))
    barrier = pltpu.get_barrier_semaphore()
    for dev in (sibling, peer(0, 1), peer(0, -1), peer(1, 1), peer(1, -1), *zring):
        pl.semaphore_signal(barrier, inc=1, device_id=dev, device_id_type=MESH)

    def load(tile, xq, half, dst, sem):
        cols = pl.ds(tile * CW, CW)
        base = xq * 32 + half * 16
        pltpu.make_async_copy(pin.at[:, pl.ds(base, 16), :, cols], dst.at[tile, xq, :, pl.ds(1, 16)], sem.at[tile, xq]).start()
        low = jnp.maximum(base - 1, 0)
        pltpu.make_async_copy(pin.at[:, pl.ds(low, 1), :, cols], dst.at[tile, xq, :, pl.ds(0, 1)], sem.at[tile, xq]).start()
        high = jnp.minimum(base + 16, 63)
        pltpu.make_async_copy(pin.at[:, pl.ds(high, 1), :, cols], dst.at[tile, xq, :, pl.ds(17, 1)], sem.at[tile, xq]).start()

    far, near = 1 - xh, xh
    ORDER = ((0, far), (1, far), (0, near), (1, near), (2, near), (2, far), (3, near), (3, far))

    def load_both(k):
        for tile, xq in ORDER[k:k + 2]:
            load(tile, xq, other, give, give_sem)
        for tile, xq in ORDER[k:k + 2]:
            load(tile, xq, core, mine, mine_sem)

    load_both(0)
    load_both(2)
    pl.semaphore_wait(barrier, 7)

    def token(k, devices):
        for dev in devices:
            pl.semaphore_signal(tok.at[k], inc=1, device_id=dev, device_id_type=MESH)

    def pass_token(k):
        pl.semaphore_wait(tok.at[k], 2 if k < 3 else 1)
        if k < 3:
            token(k + 1, zring if k < 2 else (sibling,))

    def remote(src, dst, ss, rs, dev):
        return pltpu.make_async_remote_copy(src_ref=src, dst_ref=dst, send_sem=ss, recv_sem=rs, device_id=dev,
                                            device_id_type=MESH)

    def send(src, dst, ss, rs, dev):
        remote(src, dst, ss, rs, dev).start()

    def send_if(cond, src, dst, ss, rs, dev):
        @pl.when(cond)
        def _():
            remote(src, dst, ss, rs, dev).start()

    def wait_in(dst, rs):
        pltpu.make_async_copy(dst, dst, rs).wait()

    def hand_over(k):
        for tile, xq in ORDER[k:k + 2]:
            wait_in(give.at[tile, xq], give_sem.at[tile, xq])
            send(give.at[tile, xq], theirs.at[tile, xq], snd.at[0], th_r.at[tile, xq], sibling)

    hand_over(0)
    load_both(4)
    hand_over(2)
    load_both(6)
    token(0, zring)
    for tile in range(NT):
        for xq in range(2):
            psum[tile, 0, xq] = jnp.zeros((144, CW), F32)
            psum[tile, 9, xq] = jnp.zeros((144, CW), F32)

    lane = lax.broadcasted_iota(jnp.int32, (64, CW), 1)

    def pair(k):
        for tile, xq in ORDER[k:k + 2]:
            wait_in(mine.at[tile, xq], mine_sem.at[tile, xq])
            wait_in(theirs.at[tile, xq], th_r.at[tile, xq])
            low = jnp.where(jnp.logical_and(core == 0, xq == 0), 0.0, 1.0).astype(F32)
            high = jnp.where(jnp.logical_and(core == 1, xq == 1), 0.0, 1.0).astype(F32)

            @pl.loop(0, 8, unroll=4)
            def _(d):
                v = (mine[tile, xq, d].astype(F32) + theirs[tile, xq, d].astype(F32)).reshape(144, CW)
                psum[tile, d + 1, xq, 8:136] = v[8:136]
                psum[tile, d + 1, xq, 0:8] = v[0:8] * low
                psum[tile, d + 1, xq, 136:144] = v[136:144] * high

    def stencil(tile, g, xq):
        ch = TILES.index(tile) if tile != ZTILE else None

        @pl.loop(0, 4, unroll=UNROLL)
        def _(q):
            d = 2 * q + g + 1
            for hf in range(2):
                lo = hf * 64 + 8
                mid = slice(lo, lo + 64)
                c = psum[tile, d, xq, mid]
                before = psum[tile - 1, d, xq, mid] if tile > 0 else 0.0
                after = psum[tile + 1, d, xq, mid] if tile < NT - 1 else 0.0
                n = psum[tile, d, xq, slice(lo - 1, lo + 63)] + psum[tile, d, xq, slice(lo + 1, lo + 65)]
                n = n + (psum[tile, d - 1, xq, mid] + psum[tile, d + 1, xq, mid])
                n = n + (pltpu.roll(jnp.where(lane == CW - 1, before, c), 1, 1) +
                         pltpu.roll(jnp.where(lane == 0, after, c), CW - 1, 1))
                r = (6.0 * c - n).reshape(8, 8, CW)
                if tile == ZTILE:
                    for j in range(8):
                        LC[g, hf * 2 + j // 4, lax.rem(q, 2), (q // 2) * 8 + xq * 4 + j % 4] = r[j]
                elif g == 0:
                    L[0, ch, xq * 2 + q // 2, lax.rem(q, 2), pl.ds(hf * 8, 8)] = r
                else:
                    for j in range(8):
                        L[1, ch, j % 4, lax.rem(q, 2), (q // 2) * 8 + xq * 4 + hf * 2 + j // 4] = r[j]

    def relay(g, ch):
        for d, step in DIRS:
            send(L.at[g, ch, pos(g, 2), d], rel.at[g, ch, d], snd.at[1], rel_r.at[g, ch], peer(g, step))

    def direct(g, ch):
        for d, step in DIRS:
            send(L.at[g, ch, pos(g, step), 1 - d], inn.at[g, ch, 0, d], snd.at[2], in_r.at[g, ch], peer(g, step))

    def combine(g, ch):
        wait_in(rel.at[g, ch], rel_r.at[g, ch])
        for d, step in DIRS:
            rel[g, ch, d] = rel[g, ch, d] + L[g, ch, pos(g, step), d]
            send(rel.at[g, ch, d], inn.at[g, ch, 1, d], snd.at[2], in_r.at[g, ch], peer(g, step))

    def first_sum(g, ch):
        wait_in(inn.at[g, ch], in_r.at[g, ch])
        for h in range(2):
            total = (L[g, ch, pos(g, 0), h] + inn[g, ch, 0, 1 - h]) + inn[g, ch, 1, h]
            for j in range(16):
                if g == 0:
                    S[g, ch, j % 4, h, j // 4] = total[j]
                else:
                    S[g, ch, (j // 4 % 2) * 2 + j // 8, h, j % 4] = total[j]

    def second_send(g, ch):
        o = 1 - g
        if ch > 0:
            for j, step in enumerate((2, 1, -1)):
                send(S.at[g, ch, pos(o, step)], qall.at[g, ch - 1, j], snd.at[5], qall_r.at[g, ch - 1], peer(o, step))
            return
        for d, step in DIRS:
            send(S.at[g, ch, pos(o, 2), d], qrel.at[g, ch, d], snd.at[3], qrel_r.at[g, ch], peer(o, step))
        for d, step in DIRS:
            send(S.at[g, ch, pos(o, step), 1 - d], qinn.at[g, ch, 0, d], snd.at[4], qin_r.at[g, ch], peer(o, step))

    def second_combine(g, ch):
        o = 1 - g
        wait_in(qrel.at[g, ch], qrel_r.at[g, ch])
        for d, step in DIRS:
            qrel[g, ch, d] = qrel[g, ch, d] + S[g, ch, pos(o, step), d]
            send(qrel.at[g, ch, d], qinn.at[g, ch, 1, d], snd.at[4], qin_r.at[g, ch], peer(o, step))

    def second_sum(g, ch):
        own = S[g, ch, pos(1 - g, 0)]
        if ch > 0:
            wait_in(qall.at[g, ch - 1], qall_r.at[g, ch - 1])
            total = (own + qall[g, ch - 1, 0]) + (qall[g, ch - 1, 1] + qall[g, ch - 1, 2])
            for h in range(2):
                for j in range(4):
                    T[ch, h, j, g] = total[h, j]
            return
        wait_in(qinn.at[g, ch], qin_r.at[g, ch])
        for h in range(2):
            total = (own[h] + qinn[g, ch, 0, 1 - h]) + qinn[g, ch, 1, h]
            for j in range(4):
                T[ch, h, j, g] = total[j]

    def third_send(ch):
        for k in (0, 2, 1, 3):
            j = lax.rem(z + k, 4)
            zq = core * 4 + j
            for cq in range(2):
                send_if(jnp.logical_or(zq != z, core != cq), T.at[ch, cq, j], zin.at[ch, z], snd.at[6], z_r.at[ch],
                        at(X, zq, y, cq))

        @pl.when(holds)
        def _():
            zin[ch, z] = T[ch, core, lax.rem(z, 4)]

    def third_sum(ch):
        @pl.when(holds)
        def _():
            wait_in(zin.at[ch, pl.ds(0, 7)], z_r.at[ch])

        @pl.when(jnp.logical_not(holds))
        def _():
            wait_in(zin.at[ch], z_r.at[ch])

        total = (zin[ch, 0] + zin[ch, 1]) + (zin[ch, 2] + zin[ch, 3])
        total = total + ((zin[ch, 4] + zin[ch, 5]) + (zin[ch, 6] + zin[ch, 7]))
        out[:, :, TILES[ch] * CW:(TILES[ch] + 1) * CW] = total * scale

    def z_active(j, step):
        dest = wrap(z + step * (5 - j), 8)
        return dest // 4 == core, lax.rem(dest, 4)

    def z_part(j, short):
        for g in range(2):
            for d, step in DIRS:
                active, block = z_active(j, step)
                cq = 1 - d if short else d

                @pl.when(active)
                def _():
                    if j > 1 + short:
                        wait_in(zc.at[d, j - 2, g, cq], zc_r.at[d, j - 2, g, cq])
                        LC[g, block, cq] = LC[g, block, cq] + zc[d, j - 2, g, cq]
                    send(LC.at[g, block, cq], zc.at[d, j - 1, g, cq], zc_s.at[d, j - 1], zc_r.at[d, j - 1, g, cq], zring[d])

    def z_final():
        block = lax.rem(z, 4)

        @pl.when(holds)
        def _():
            for g in range(2):
                for d in range(2):
                    for cq in range(2):
                        wait_in(zc.at[d, 3, g, cq], zc_r.at[d, 3, g, cq])

                @pl.loop(0, 16)
                def _(i):
                    for cq in range(2):
                        R[cq * 16 + i, g] = (LC[g, block, cq, i] + zc[0, 3, g, cq, i]) + zc[1, 3, g, cq, i]

            xyin[me] = R[core * 16 + lax.rem(X, 2) * 8 + (X // 2) * 4 + y]
            for a in (2, 1, 3, 0):
                for b in (2, 1, 3, 0):
                    Xq, yq = wrap(X + a, 4), wrap(y + b, 4)
                    i = lax.rem(Xq, 2) * 8 + (Xq // 2) * 4 + yq
                    for cq in range(2):
                        if a or b:
                            send(R.at[cq * 16 + i], xyin.at[me], snd.at[7], xy_r, at(Xq, z, yq, cq))
                        else:
                            send_if(core != cq, R.at[cq * 16 + i], xyin.at[me], snd.at[7], xy_r, at(Xq, z, yq, cq))

    def xy_sum():
        @pl.when(holds)
        def _():
            wait_in(xyin.at[pl.ds(0, 15)], xy_r)

        @pl.when(jnp.logical_not(holds))
        def _():
            wait_in(xyin, xy_r)

        parts = [xyin[k] for k in range(16)]
        while len(parts) > 1:
            parts = [parts[k] + parts[k + 1] for k in range(0, len(parts), 2)]
        out[:, :, ZTILE * CW:(ZTILE + 1) * CW] = parts[0] * scale

    def each(fn, ch):
        for g in range(2):
            fn(g, ch)

    def begin(ch):
        for g in range(2):
            for xq in range(2):
                stencil(TILES[ch], g, xq)
            relay(g, ch)

    pair(0)
    stencil(0, 0, far)
    relay(0, 0)
    hand_over(4)
    stencil(0, 1, far)
    pair(2)
    stencil(0, 1, near)
    relay(1, 0)
    direct(1, 0)
    stencil(0, 0, near)
    direct(0, 0)
    hand_over(6)
    pair(4)
    stencil(ZTILE, 0, 0)
    stencil(ZTILE, 0, 1)
    stencil(ZTILE, 1, 0)
    stencil(ZTILE, 1, 1)
    z_part(1, 0)
    pair(6)
    begin(1)
    z_part(2, 1)
    combine(0, 0)
    direct(0, 1)
    combine(1, 0)
    direct(1, 1)
    pass_token(0)
    begin(2)
    z_part(2, 0)
    each(combine, 1)
    each(direct, 2)
    pass_token(1)
    z_part(3, 1)
    each(first_sum, 0)
    each(second_send, 0)
    z_part(3, 0)
    each(combine, 2)
    pass_token(2)
    z_part(4, 1)
    each(first_sum, 1)
    each(second_send, 1)
    z_part(4, 0)
    each(second_combine, 0)
    each(first_sum, 2)
    each(second_send, 2)
    each(second_sum, 0)
    pass_token(3)
    third_send(0)
    z_final()
    each(second_sum, 1)
    third_send(1)
    each(second_sum, 2)
    third_send(2)
    third_sum(0)
    third_sum(1)
    xy_sum()
    third_sum(2)
    for k, buffer in enumerate((theirs, rel, inn, qrel, qinn, qall)):
        wait_in(buffer, snd.at[k])

    @pl.when(holds)
    def _():
        wait_in(zin.at[:, pl.ds(0, 7)], snd.at[6])
        wait_in(R.at[pl.ds(0, 31)], snd.at[7])

    @pl.when(jnp.logical_not(holds))
    def _():
        wait_in(zin, snd.at[6])

    for j in range(1, 5):
        for d, step in DIRS:
            @pl.when(z_active(j, step)[0])
            def _():
                sent = zc.at[d, 0, 0] if j == 1 else zc.at[d, j - 1]
                wait_in(sent, zc_s.at[d, j - 1])


def solution(mesh):
    shots = mesh.shape["shot"] * mesh.shape["tile"]
    scale = 1.0 / float(shots) ** 0.5
    D = pltpu.SemaphoreType.DMA
    V = pltpu.VMEM

    def step(partials):
        return pl.pallas_call(
            functools.partial(kernel, scale),
            out_shape=jax.ShapeDtypeStruct((2, 8, NY), F32),
            in_specs=[pl.BlockSpec(memory_space=pl.ANY)],
            out_specs=pl.BlockSpec(memory_space=pltpu.VMEM),
            scratch_shapes=[
                V((NT, 2, 8, 18, 8, CW), BF16),
                V((NT, 2, 8, 18, 8, CW), BF16),
                V((NT, 2, 8, 18, 8, CW), BF16),
                V((NT, 10, 2, 144, CW), F32),
                V((2, NCH, 4, 2, 16, 8, CW), F32),
                V((2, NCH, 2, 16, 8, CW), F32),
                V((2, NCH, 2, 2, 16, 8, CW), F32),
                V((2, NCH, 4, 2, 4, 8, CW), F32),
                V((2, 1, 2, 4, 8, CW), F32),
                V((2, 1, 2, 2, 4, 8, CW), F32),
                V((2, 2, 3, 2, 4, 8, CW), F32),
                V((NCH, 2, 4, 2, 8, CW), F32),
                V((NCH, 8, 2, 8, CW), F32),
                V((2, 4, 2, 16, 8, CW), F32),
                V((2, 4, 2, 2, 16, 8, CW), F32),
                V((32, 2, 8, CW), F32),
                V((16, 2, 8, CW), F32),
                D((NT, 2)), D((NT, 2)), D((NT, 2)),
                D((2, NCH)), D((2, NCH)),
                D((2, 1)), D((2, 1)), D((2, 2)),
                D((NCH,)), D((2, 4, 2, 2)), D(()),
                D((8,)), D((2, 4)),
                pltpu.SemaphoreType.REGULAR((4,)),
            ],
            compiler_params=pltpu.CompilerParams(collective_id=0, has_side_effects=True,
                                                 vmem_limit_bytes=52 * 1024 * 1024),
        )(partials.reshape(8, 64, 8, NY))

    return jax.shard_map(step, mesh=mesh, in_specs=(P(("shot", "tile"), None, None, None),),
                         out_specs=P("shot", "tile", None), check_vma=False)
```

```python
import functools

import jax
import jax.numpy as jnp
from jax import lax
from jax.experimental import pallas as pl
from jax.experimental.pallas import tpu as pltpu
from jax.sharding import PartitionSpec as P

MESH = pl.DeviceIdType.MESH
NY = 512
CW = 128
NT = NY // CW
TILES = (0, 2, 3)
ZTILE = 1
NCH = len(TILES)
UNROLL = 4
F32 = jnp.float32
BF16 = jnp.bfloat16


def kernel(scale, pin, out, give, mine, theirs, psum, L, rel, inn, S, qrel, qinn, qall, T, zin, LC, zc, R, xyin,
           give_sem, mine_sem, th_r, rel_r, in_r, qrel_r, qin_r, qall_r, z_r, zc_r, xy_r, snd, zc_s, tok):
    s, t = lax.axis_index("shot"), lax.axis_index("tile")
    core, xl = lax.rem(s, 2), s // 2
    xh, z, y = t // 32, lax.rem(t // 4, 8), lax.rem(t, 4)
    X = xh * 2 + xl
    other = 1 - core
    holds = z // 4 == core
    me = X * 4 + y
    DIRS = tuple(enumerate((1, -1)))

    def at(Xq, zq, yq, cq):
        return (lax.rem(Xq, 2) * 2 + cq, (Xq // 2) * 32 + zq * 4 + yq)

    def wrap(v, n):
        return lax.rem(v + n, n)

    def pos(g, step):
        return wrap((X if g == 0 else y) + step, 4)

    def peer(g, step):
        return at(pos(0, step), z, y, core) if g == 0 else at(X, z, pos(1, step), core)

    sibling = at(X, z, y, other)
    zring = (at(X, wrap(z + 1, 8), y, core), at(X, wrap(z - 1, 8), y, core))
    barrier = pltpu.get_barrier_semaphore()
    for dev in (sibling, peer(0, 1), peer(0, -1), peer(1, 1), peer(1, -1), *zring):
        pl.semaphore_signal(barrier, inc=1, device_id=dev, device_id_type=MESH)

    def load(tile, xq, half, dst, sem):
        cols = pl.ds(tile * CW, CW)
        base = xq * 32 + half * 16
        pltpu.make_async_copy(pin.at[:, pl.ds(base, 16), :, cols], dst.at[tile, xq, :, pl.ds(1, 16)], sem.at[tile, xq]).start()
        low = jnp.maximum(base - 1, 0)
        pltpu.make_async_copy(pin.at[:, pl.ds(low, 1), :, cols], dst.at[tile, xq, :, pl.ds(0, 1)], sem.at[tile, xq]).start()
        high = jnp.minimum(base + 16, 63)
        pltpu.make_async_copy(pin.at[:, pl.ds(high, 1), :, cols], dst.at[tile, xq, :, pl.ds(17, 1)], sem.at[tile, xq]).start()

    far, near = 1 - xh, xh
    ORDER = ((0, far), (1, far), (0, near), (1, near), (2, near), (2, far), (3, near), (3, far))

    def load_both(k):
        for tile, xq in ORDER[k:k + 2]:
            load(tile, xq, other, give, give_sem)
        for tile, xq in ORDER[k:k + 2]:
            load(tile, xq, core, mine, mine_sem)

    load_both(0)
    load_both(2)
    pl.semaphore_wait(barrier, 7)

    def token(k, devices):
        for dev in devices:
            pl.semaphore_signal(tok.at[k], inc=1, device_id=dev, device_id_type=MESH)

    def pass_token(k):
        pl.semaphore_wait(tok.at[k], 2 if k < 3 else 1)
        if k < 3:
            token(k + 1, zring if k < 2 else (sibling,))

    def remote(src, dst, ss, rs, dev):
        return pltpu.make_async_remote_copy(src_ref=src, dst_ref=dst, send_sem=ss, recv_sem=rs, device_id=dev,
                                            device_id_type=MESH)

    def send(src, dst, ss, rs, dev):
        remote(src, dst, ss, rs, dev).start()

    def send_if(cond, src, dst, ss, rs, dev):
        @pl.when(cond)
        def _():
            remote(src, dst, ss, rs, dev).start()

    def wait_in(dst, rs):
        pltpu.make_async_copy(dst, dst, rs).wait()

    def hand_over(k):
        for tile, xq in ORDER[k:k + 2]:
            wait_in(give.at[tile, xq], give_sem.at[tile, xq])
            send(give.at[tile, xq], theirs.at[tile, xq], snd.at[0], th_r.at[tile, xq], sibling)

    hand_over(0)
    load_both(4)
    hand_over(2)
    load_both(6)
    token(0, zring)
    for tile in range(NT):
        for xq in range(2):
            psum[tile, 0, xq] = jnp.zeros((144, CW), F32)
            psum[tile, 9, xq] = jnp.zeros((144, CW), F32)

    lane = lax.broadcasted_iota(jnp.int32, (64, CW), 1)

    def pair(k):
        for tile, xq in ORDER[k:k + 2]:
            wait_in(mine.at[tile, xq], mine_sem.at[tile, xq])
            wait_in(theirs.at[tile, xq], th_r.at[tile, xq])
            low = jnp.where(jnp.logical_and(core == 0, xq == 0), 0.0, 1.0).astype(F32)
            high = jnp.where(jnp.logical_and(core == 1, xq == 1), 0.0, 1.0).astype(F32)

            @pl.loop(0, 8, unroll=4)
            def _(d):
                v = (mine[tile, xq, d].astype(F32) + theirs[tile, xq, d].astype(F32)).reshape(144, CW)
                psum[tile, d + 1, xq, 8:136] = v[8:136]
                psum[tile, d + 1, xq, 0:8] = v[0:8] * low
                psum[tile, d + 1, xq, 136:144] = v[136:144] * high

    def stencil(tile, g, xq):
        ch = TILES.index(tile) if tile != ZTILE else None

        @pl.loop(0, 4, unroll=UNROLL)
        def _(q):
            d = 2 * q + g + 1
            for hf in range(2):
                lo = hf * 64 + 8
                mid = slice(lo, lo + 64)
                c = psum[tile, d, xq, mid]
                before = psum[tile - 1, d, xq, mid] if tile > 0 else 0.0
                after = psum[tile + 1, d, xq, mid] if tile < NT - 1 else 0.0
                n = psum[tile, d, xq, slice(lo - 1, lo + 63)] + psum[tile, d, xq, slice(lo + 1, lo + 65)]
                n = n + (psum[tile, d - 1, xq, mid] + psum[tile, d + 1, xq, mid])
                n = n + (pltpu.roll(jnp.where(lane == CW - 1, before, c), 1, 1) +
                         pltpu.roll(jnp.where(lane == 0, after, c), CW - 1, 1))
                r = (6.0 * c - n).reshape(8, 8, CW)
                if tile == ZTILE:
                    for j in range(8):
                        LC[g, hf * 2 + j // 4, lax.rem(q, 2), (q // 2) * 8 + xq * 4 + j % 4] = r[j]
                elif g == 0:
                    L[0, ch, xq * 2 + q // 2, lax.rem(q, 2), pl.ds(hf * 8, 8)] = r
                else:
                    for j in range(8):
                        L[1, ch, j % 4, lax.rem(q, 2), (q // 2) * 8 + xq * 4 + hf * 2 + j // 4] = r[j]

    def relay(g, ch):
        for d, step in DIRS:
            send(L.at[g, ch, pos(g, 2), d], rel.at[g, ch, d], snd.at[1], rel_r.at[g, ch], peer(g, step))

    def direct(g, ch):
        for d, step in DIRS:
            send(L.at[g, ch, pos(g, step), 1 - d], inn.at[g, ch, 0, d], snd.at[2], in_r.at[g, ch], peer(g, step))

    def combine(g, ch):
        wait_in(rel.at[g, ch], rel_r.at[g, ch])
        for d, step in DIRS:
            rel[g, ch, d] = rel[g, ch, d] + L[g, ch, pos(g, step), d]
            send(rel.at[g, ch, d], inn.at[g, ch, 1, d], snd.at[2], in_r.at[g, ch], peer(g, step))

    def first_sum(g, ch):
        wait_in(inn.at[g, ch], in_r.at[g, ch])
        for h in range(2):
            total = (L[g, ch, pos(g, 0), h] + inn[g, ch, 0, 1 - h]) + inn[g, ch, 1, h]
            for j in range(16):
                if g == 0:
                    S[g, ch, j % 4, h, j // 4] = total[j]
                else:
                    S[g, ch, (j // 4 % 2) * 2 + j // 8, h, j % 4] = total[j]

    def second_send(g, ch):
        o = 1 - g
        if ch == NCH - 1:
            for h in range(2):
                for j, step in enumerate((2, 1, -1)):
                    send(S.at[g, ch, pos(o, step), h], qall.at[g, ch - 1, j, h], snd.at[5], qall_r.at[g, ch - 1 + h],
                         peer(o, step))
            return
        if ch > 0:
            for j, step in enumerate((2, 1, -1)):
                send(S.at[g, ch, pos(o, step)], qall.at[g, ch - 1, j], snd.at[5], qall_r.at[g, ch - 1], peer(o, step))
            return
        for d, step in DIRS:
            send(S.at[g, ch, pos(o, 2), d], qrel.at[g, ch, d], snd.at[3], qrel_r.at[g, ch], peer(o, step))
        for d, step in DIRS:
            send(S.at[g, ch, pos(o, step), 1 - d], qinn.at[g, ch, 0, d], snd.at[4], qin_r.at[g, ch], peer(o, step))

    def second_combine(g, ch):
        o = 1 - g
        wait_in(qrel.at[g, ch], qrel_r.at[g, ch])
        for d, step in DIRS:
            qrel[g, ch, d] = qrel[g, ch, d] + S[g, ch, pos(o, step), d]
            send(qrel.at[g, ch, d], qinn.at[g, ch, 1, d], snd.at[4], qin_r.at[g, ch], peer(o, step))

    def second_sum(g, ch):
        own = S[g, ch, pos(1 - g, 0)]
        if ch > 0:
            wait_in(qall.at[g, ch - 1], qall_r.at[g, ch - 1])
            total = (own + qall[g, ch - 1, 0]) + (qall[g, ch - 1, 1] + qall[g, ch - 1, 2])
            for h in range(2):
                for j in range(4):
                    T[ch, h, j, g] = total[h, j]
            return
        wait_in(qinn.at[g, ch], qin_r.at[g, ch])
        for h in range(2):
            total = (own[h] + qinn[g, ch, 0, 1 - h]) + qinn[g, ch, 1, h]
            for j in range(4):
                T[ch, h, j, g] = total[j]

    def last_sum(h):
        k = NCH - 2
        for g in range(2):
            wait_in(qall.at[g, k, :, h], qall_r.at[g, k + h])
            total = (S[g, NCH - 1, pos(1 - g, 0), h] + qall[g, k, 0, h]) + (qall[g, k, 1, h] + qall[g, k, 2, h])
            for j in range(4):
                T[NCH - 1, h, j, g] = total[j]

    def third_send(ch, cores=(0, 1)):
        for k in (0, 2, 1, 3):
            j = lax.rem(z + k, 4)
            zq = core * 4 + j
            for cq in cores:
                send_if(jnp.logical_or(zq != z, core != cq), T.at[ch, cq, j], zin.at[ch, z], snd.at[6], z_r.at[ch],
                        at(X, zq, y, cq))

        if 1 in cores:
            @pl.when(holds)
            def _():
                zin[ch, z] = T[ch, core, lax.rem(z, 4)]

    def third_sum(ch):
        @pl.when(holds)
        def _():
            wait_in(zin.at[ch, pl.ds(0, 7)], z_r.at[ch])

        @pl.when(jnp.logical_not(holds))
        def _():
            wait_in(zin.at[ch], z_r.at[ch])

        total = (zin[ch, 0] + zin[ch, 1]) + (zin[ch, 2] + zin[ch, 3])
        total = total + ((zin[ch, 4] + zin[ch, 5]) + (zin[ch, 6] + zin[ch, 7]))
        out[:, :, TILES[ch] * CW:(TILES[ch] + 1) * CW] = total * scale

    def z_active(j, step):
        dest = wrap(z + step * (5 - j), 8)
        return dest // 4 == core, lax.rem(dest, 4)

    def z_part(j, short):
        for g in range(2):
            for d, step in DIRS:
                active, block = z_active(j, step)
                cq = 1 - d if short else d

                @pl.when(active)
                def _():
                    if j > 1 + short:
                        wait_in(zc.at[d, j - 2, g, cq], zc_r.at[d, j - 2, g, cq])
                        LC[g, block, cq] = LC[g, block, cq] + zc[d, j - 2, g, cq]
                    send(LC.at[g, block, cq], zc.at[d, j - 1, g, cq], zc_s.at[d, j - 1], zc_r.at[d, j - 1, g, cq], zring[d])

    def z_final():
        block = lax.rem(z, 4)

        @pl.when(holds)
        def _():
            for g in range(2):
                for d in range(2):
                    for cq in range(2):
                        wait_in(zc.at[d, 3, g, cq], zc_r.at[d, 3, g, cq])

                @pl.loop(0, 16)
                def _(i):
                    for cq in range(2):
                        R[cq * 16 + i, g] = (LC[g, block, cq, i] + zc[0, 3, g, cq, i]) + zc[1, 3, g, cq, i]

            xyin[me] = R[core * 16 + lax.rem(X, 2) * 8 + (X // 2) * 4 + y]
            for a in (2, 1, 3, 0):
                for b in (2, 1, 3, 0):
                    Xq, yq = wrap(X + a, 4), wrap(y + b, 4)
                    i = lax.rem(Xq, 2) * 8 + (Xq // 2) * 4 + yq
                    for cq in range(2):
                        if a or b:
                            send(R.at[cq * 16 + i], xyin.at[me], snd.at[7], xy_r, at(Xq, z, yq, cq))
                        else:
                            send_if(core != cq, R.at[cq * 16 + i], xyin.at[me], snd.at[7], xy_r, at(Xq, z, yq, cq))

    def xy_sum():
        @pl.when(holds)
        def _():
            wait_in(xyin.at[pl.ds(0, 15)], xy_r)

        @pl.when(jnp.logical_not(holds))
        def _():
            wait_in(xyin, xy_r)

        parts = [xyin[k] for k in range(16)]
        while len(parts) > 1:
            parts = [parts[k] + parts[k + 1] for k in range(0, len(parts), 2)]
        out[:, :, ZTILE * CW:(ZTILE + 1) * CW] = parts[0] * scale

    def each(fn, ch):
        for g in range(2):
            fn(g, ch)

    def begin(ch):
        for g in range(2):
            for xq in range(2):
                stencil(TILES[ch], g, xq)
            relay(g, ch)

    pair(0)
    stencil(0, 0, far)
    relay(0, 0)
    hand_over(4)
    stencil(0, 1, far)
    pair(2)
    stencil(0, 1, near)
    relay(1, 0)
    direct(1, 0)
    stencil(0, 0, near)
    direct(0, 0)
    hand_over(6)
    pair(4)
    stencil(ZTILE, 0, 0)
    stencil(ZTILE, 0, 1)
    stencil(ZTILE, 1, 0)
    stencil(ZTILE, 1, 1)
    z_part(1, 0)
    pair(6)
    begin(1)
    z_part(2, 1)
    combine(0, 0)
    direct(0, 1)
    combine(1, 0)
    direct(1, 1)
    pass_token(0)
    begin(2)
    z_part(2, 0)
    each(combine, 1)
    each(direct, 2)
    pass_token(1)
    z_part(3, 1)
    each(first_sum, 0)
    each(second_send, 0)
    z_part(3, 0)
    each(combine, 2)
    pass_token(2)
    z_part(4, 1)
    each(first_sum, 1)
    each(second_send, 1)
    z_part(4, 0)
    each(second_combine, 0)
    each(first_sum, 2)
    each(second_send, 2)
    each(second_sum, 0)
    pass_token(3)
    third_send(0)
    z_final()
    each(second_sum, 1)
    third_send(1)
    for h in range(2):
        last_sum(h)
        third_send(2, (h,))
    third_sum(0)
    third_sum(1)
    xy_sum()
    third_sum(2)
    for k, buffer in enumerate((theirs, rel, inn, qrel, qinn, qall)):
        wait_in(buffer, snd.at[k])

    @pl.when(holds)
    def _():
        wait_in(zin.at[:, pl.ds(0, 7)], snd.at[6])
        wait_in(R.at[pl.ds(0, 31)], snd.at[7])

    @pl.when(jnp.logical_not(holds))
    def _():
        wait_in(zin, snd.at[6])

    for j in range(1, 5):
        for d, step in DIRS:
            @pl.when(z_active(j, step)[0])
            def _():
                sent = zc.at[d, 0, 0] if j == 1 else zc.at[d, j - 1]
                wait_in(sent, zc_s.at[d, j - 1])


def solution(mesh):
    shots = mesh.shape["shot"] * mesh.shape["tile"]
    scale = 1.0 / float(shots) ** 0.5
    D = pltpu.SemaphoreType.DMA
    V = pltpu.VMEM

    def step(partials):
        return pl.pallas_call(
            functools.partial(kernel, scale),
            out_shape=jax.ShapeDtypeStruct((2, 8, NY), F32),
            in_specs=[pl.BlockSpec(memory_space=pl.ANY)],
            out_specs=pl.BlockSpec(memory_space=pltpu.VMEM),
            scratch_shapes=[
                V((NT, 2, 8, 18, 8, CW), BF16),
                V((NT, 2, 8, 18, 8, CW), BF16),
                V((NT, 2, 8, 18, 8, CW), BF16),
                V((NT, 10, 2, 144, CW), F32),
                V((2, NCH, 4, 2, 16, 8, CW), F32),
                V((2, NCH, 2, 16, 8, CW), F32),
                V((2, NCH, 2, 2, 16, 8, CW), F32),
                V((2, NCH, 4, 2, 4, 8, CW), F32),
                V((2, 1, 2, 4, 8, CW), F32),
                V((2, 1, 2, 2, 4, 8, CW), F32),
                V((2, 2, 3, 2, 4, 8, CW), F32),
                V((NCH, 2, 4, 2, 8, CW), F32),
                V((NCH, 8, 2, 8, CW), F32),
                V((2, 4, 2, 16, 8, CW), F32),
                V((2, 4, 2, 2, 16, 8, CW), F32),
                V((32, 2, 8, CW), F32),
                V((16, 2, 8, CW), F32),
                D((NT, 2)), D((NT, 2)), D((NT, 2)),
                D((2, NCH)), D((2, NCH)),
                D((2, 1)), D((2, 1)), D((2, 3)),
                D((NCH,)), D((2, 4, 2, 2)), D(()),
                D((8,)), D((2, 4)),
                pltpu.SemaphoreType.REGULAR((4,)),
            ],
            compiler_params=pltpu.CompilerParams(collective_id=0, has_side_effects=True,
                                                 vmem_limit_bytes=52 * 1024 * 1024),
        )(partials.reshape(8, 64, 8, NY))

    return jax.shard_map(step, mesh=mesh, in_specs=(P(("shot", "tile"), None, None, None),),
                         out_specs=P("shot", "tile", None), check_vma=False)
```
